8 devices in a mesh: mat: 2 (over z, y), row: 4 (over x, core).
Axes of the slice: x: 2, y: 2, z: 1, core: 2. Of those that a mesh axis runs over, the one named last changes fastest.
Arguments:
- a_mat: bfloat16 [28672, 1024], P(('mat', 'row')), parts along dimension 0
Outputs:
- output: float32 [8, 3, 3584, 3584], P(('mat', 'row')), parts along dimension 0
There are 2 independent parts. The reference program is written for one: setup_inputs(seed, part) draws one part's arguments, and reference() takes and returns one part's arrays. A program takes and returns all parts, laid end to end along the dimension named above; each array names one.
All inputs are finite; a program needn't handle non-finite values.
Results may differ from the reference program's by a relative error of at most 0.001.
Values are sent between devices in bfloat16 or wider.
A program may use at most 1 GiB of HBM per device.

```python
import math
import jax
import jax.numpy as jnp
import numpy as np
from jax import lax

ORDER_N = 14336
INNER_K = 1024
GROUP_SIZE = 4
BLOCK_ROWS = ORDER_N // GROUP_SIZE


def slot_offsets(group_size):
    half_group = group_size // 2
    low_count = 2 ** (int(math.log2(half_group)) // 2)
    low_off = [low_count - 1 - (slot_idx - 1) % low_count for slot_idx in range(1, half_group + 1)]
    high_off = [((slot_idx - 1) // low_count + 1) * low_count for slot_idx in range(1, half_group + 1)]
    return low_off, high_off


def setup_inputs(seed: int = 0, part: int = 0) -> dict:
    base_key = jax.random.fold_in(jax.random.key(seed), part)
    key_vals, key_scale = jax.random.split(base_key)
    values = jax.random.normal(key_vals, (GROUP_SIZE, BLOCK_ROWS, INNER_K), jnp.float32)
    block_scale = jax.random.uniform(key_scale, (GROUP_SIZE, 1, 1), jnp.float32, 0.75, 1.5)
    a_mat = (values * block_scale * INNER_K ** -0.25).reshape(ORDER_N, INNER_K)
    return {"a_mat": a_mat.astype(jnp.bfloat16)}


def reference(a_mat):
    half_group = GROUP_SIZE // 2
    low_off, high_off = slot_offsets(GROUP_SIZE)
    device_ids = np.arange(GROUP_SIZE)[:, None]
    low_blk = (device_ids + np.array([0] + low_off)[None, :]) % GROUP_SIZE
    high_blk = (device_ids + np.array([0] + high_off)[None, :]) % GROUP_SIZE
    keep_slot = (np.arange(half_group + 1)[None, :] < half_group) | (low_blk < half_group)
    big_blk = np.maximum(low_blk, high_blk).reshape(-1).astype(np.int32)
    small_blk = np.minimum(low_blk, high_blk).reshape(-1).astype(np.int32)
    blocks = a_mat.reshape(GROUP_SIZE, BLOCK_ROWS, INNER_K)

    def block_product(blk_pair):
        left_blk = lax.dynamic_index_in_dim(blocks, blk_pair[0], 0, keepdims=False)
        right_blk = lax.dynamic_index_in_dim(blocks, blk_pair[1], 0, keepdims=False)
        return jnp.dot(left_blk, right_blk.T, preferred_element_type=jnp.float32)

    products = lax.map(block_product, (jnp.asarray(big_blk), jnp.asarray(small_blk)))
    products = products.reshape(GROUP_SIZE, half_group + 1, BLOCK_ROWS, BLOCK_ROWS)
    return jnp.where(jnp.asarray(keep_slot)[:, :, None, None], products, 0.0)
```

```python
import functools

import jax
import jax.numpy as jnp
from jax import lax
from jax.experimental import pallas as pl
from jax.experimental.pallas import tpu as pltpu
from jax.sharding import PartitionSpec as P


TILE = 512
NEXT = [(1, 0), (2, 1), (3, 2), (0, 3)]
FAR = [(3, 1)]
PASS = [(1, 0)]
SUB = [(k * TILE, TILE) for k in range(6)] + [(3072, 256), (3328, 128), (3456, 128)]


def dot_t(x, y):
    return lax.dot_general(x, y, (((1,), (1,)), ((), ())), preferred_element_type=jnp.float32)


def cost(rows, cols, depth, out_bytes):
    return pl.CostEstimate(flops=2 * rows * cols * depth, bytes_accessed=out_bytes + 2 * depth * (rows + cols), transcendentals=0)


def diag_kernel(x_ref, y_ref, out_ref):
    cols = y_ref.shape[0]

    @pl.loop(0, cols // TILE)
    def _(j):
        at = pl.ds(pl.multiple_of(j * TILE, TILE), TILE)
        out_ref[0, 0, :, at] = dot_t(x_ref[...], y_ref[at, :])


def diag(a):
    rows, depth = a.shape
    return pl.pallas_call(
        diag_kernel,
        grid=(rows // TILE,),
        in_specs=[pl.BlockSpec((TILE, depth), lambda i: (i, 0)), pl.BlockSpec((rows, depth), lambda i: (0, 0))],
        out_specs=pl.BlockSpec((1, 1, TILE, rows), lambda i: (0, 0, i, 0)),
        out_shape=jax.ShapeDtypeStruct((1, 3, rows, rows), jnp.float32),
        cost_estimate=cost(rows, rows, depth, 4 * rows * rows),
        compiler_params=pltpu.CompilerParams(vmem_limit_bytes=40 << 20),
        name="diag",
    )(a, a)


def slot1_kernel(p_ref, part_ref, own_ref, _, out_ref):
    @pl.when(p_ref[0] < 3)
    def _():
        out_ref[0, 0] = dot_t(part_ref[...], own_ref[...])

    @pl.when(p_ref[0] == 3)
    def _():
        out_ref[0, 0] = dot_t(own_ref[...], part_ref[...])


def slot1(k, p, part, a, out):
    rows, depth = a.shape
    return pl.pallas_call(
        slot1_kernel,
        grid_spec=pltpu.PrefetchScalarGridSpec(
            num_scalar_prefetch=1,
            grid=(rows // TILE,),
            in_specs=[
                pl.BlockSpec((TILE, depth), lambda j, p: (0, 0)),
                pl.BlockSpec((TILE, depth), lambda j, p: (j, 0)),
                pl.BlockSpec(memory_space=pl.ANY),
            ],
            out_specs=pl.BlockSpec((1, 1, TILE, TILE), lambda j, p: (0, 1, jnp.where(p[0] == 3, j, k), jnp.where(p[0] == 3, k, j))),
        ),
        out_shape=jax.ShapeDtypeStruct(out.shape, out.dtype),
        input_output_aliases={3: 0},
        cost_estimate=cost(TILE, rows, depth, 4 * TILE * rows),
        compiler_params=pltpu.CompilerParams(vmem_limit_bytes=40 << 20),
        name="slot1",
    )(p, part, a, out)


def slot2_kernel(p_ref, near_ref, far_ref, own_ref, _, out_ref):
    @pl.when(p_ref[0] == 0)
    def _():
        out_ref[0, 0] = dot_t(near_ref[...], own_ref[...])

    @pl.when(p_ref[0] == 1)
    def _():
        out_ref[0, 0] = dot_t(far_ref[...], own_ref[...])

    @pl.when(p_ref[0] >= 2)
    def _():
        out_ref[...] = jnp.zeros_like(out_ref)


def slot2(first, size, p, near, far, a, out):
    rows, depth = a.shape
    near_blk = first % TILE // size
    out_blk = first // size
    return pl.pallas_call(
        slot2_kernel,
        grid_spec=pltpu.PrefetchScalarGridSpec(
            num_scalar_prefetch=1,
            grid=(rows // TILE,),
            in_specs=[
                pl.BlockSpec((size, depth), lambda j, p: (near_blk, 0)),
                pl.BlockSpec((size, depth), lambda j, p: (0, 0)),
                pl.BlockSpec((TILE, depth), lambda j, p: (j, 0)),
                pl.BlockSpec(memory_space=pl.ANY),
            ],
            out_specs=pl.BlockSpec((1, 1, size, TILE), lambda j, p: (0, 2, out_blk, j)),
        ),
        out_shape=jax.ShapeDtypeStruct(out.shape, out.dtype),
        input_output_aliases={4: 0},
        cost_estimate=cost(size, rows, depth, 4 * size * rows),
        compiler_params=pltpu.CompilerParams(vmem_limit_bytes=40 << 20),
        name="slot2",
    )(p, near, far, a, out)


def solution(mesh):
    assert mesh.shape["row"] == 4

    def local(a):
        rows = a.shape[0]
        p = lax.axis_index("row").astype(jnp.int32).reshape(1)
        parts = [lax.ppermute(a[k * TILE:(k + 1) * TILE], "row", NEXT) for k in range(rows // TILE)]
        out = diag(a)
        passed = [lax.ppermute(part, "row", PASS) for part in parts]
        far = [lax.ppermute(a[first:first + size], "row", FAR) for first, size in SUB]
        for k, part in enumerate(parts):
            out = slot1(k, p, part, a, out)
        for (first, size), far_part in zip(SUB, far):
            out = slot2(first, size, p, passed[first // TILE], far_part, a, out)
        return out

    return jax.shard_map(local, mesh=mesh, in_specs=(P(("mat", "row"), None),), out_specs=P(("mat", "row"), None, None, None), check_vma=False)
```

```python
import jax
import jax.numpy as jnp
from jax import lax
from jax.experimental import pallas as pl
from jax.experimental.pallas import tpu as pltpu
from jax.sharding import PartitionSpec as P


TILE = 512
NEXT = [(1, 0), (2, 1), (3, 2), (0, 3)]
FAR = [(3, 1)]
PASS = [(1, 0)]
PARTS = [(0, 512), (512, 1536), (2048, 1024), (3072, 512)]
FARS = [(0, 512), (512, 1024), (1536, 512), (2048, 1024), (3072, 256), (3328, 256)]
DEPTH = 3


def dot_t(x, y):
    return lax.dot_general(x, y, (((1,), (1,)), ((), ())), preferred_element_type=jnp.float32)


def tiles(ref, index, size):
    return ref[pl.ds(pl.multiple_of(index * size, size), size), :]


def stream(steps, buf, sem, value, place):
    def copy(s):
        return pltpu.make_async_copy(buf.at[lax.rem(s, DEPTH)], place(s), sem.at[lax.rem(s, DEPTH)])

    @pl.loop(0, steps)
    def _(s):
        @pl.when(s >= DEPTH)
        def _():
            copy(s - DEPTH).wait()

        buf[lax.rem(s, DEPTH)] = value(s)
        copy(s).start()

    for s in range(max(steps - DEPTH, 0), steps):
        copy(s).wait()


def call(kernel, rows, cols, depth, out, refs, scratch, tile):
    made = isinstance(out, jax.ShapeDtypeStruct)
    args = [a for a, _ in refs] + ([] if made else [out])
    return pl.pallas_call(
        kernel,
        in_specs=[pl.BlockSpec(memory_space=space) for _, space in refs] + ([] if made else [pl.BlockSpec(memory_space=pl.ANY)]),
        out_specs=pl.BlockSpec(memory_space=pl.ANY),
        out_shape=jax.ShapeDtypeStruct(out.shape, out.dtype),
        input_output_aliases={} if made else {len(args) - 1: 0},
        scratch_shapes=[pltpu.VMEM((DEPTH, *tile), jnp.float32), pltpu.SemaphoreType.DMA((DEPTH,)), *scratch],
        cost_estimate=pl.CostEstimate(
            flops=2 * rows * cols * depth, bytes_accessed=4 * rows * cols + 2 * rows * depth, transcendentals=0
        ),
        compiler_params=pltpu.CompilerParams(vmem_limit_bytes=24 << 20),
    )(*args)


def diag(own):
    rows, depth = own.shape

    def kernel(own_ref, out_ref, buf, sem):
        wide = rows // TILE

        def place(s):
            return out_ref.at[0, 0, pl.ds(s // wide * TILE, TILE), pl.ds(lax.rem(s, wide) * TILE, TILE)]

        def value(s):
            return dot_t(tiles(own_ref, s // wide, TILE), tiles(own_ref, lax.rem(s, wide), TILE))

        stream(wide * wide, buf, sem, value, place)

    out = jax.ShapeDtypeStruct((1, 3, rows, rows), jnp.float32)
    return call(kernel, rows, rows, depth, out, [(own, pltpu.VMEM)], [], (TILE, TILE))


def slot1(first, size, part, own, out):
    rows, depth = own.shape

    def kernel(part_ref, own_ref, _, out_ref, buf, sem, held, held_sem):
        p = lax.axis_index("row")
        load = pltpu.make_async_copy(part_ref, held, held_sem)
        load.start()
        load.wait()
        tall = size // TILE
        steps = tall * (rows // TILE)

        @pl.when(p < 3)
        def _():
            stream(
                steps, buf, sem,
                lambda s: dot_t(tiles(held, lax.rem(s, tall), TILE), tiles(own_ref, s // tall, TILE)),
                lambda s: out_ref.at[0, 1, pl.ds(first + lax.rem(s, tall) * TILE, TILE), pl.ds(s // tall * TILE, TILE)],
            )

        @pl.when(p == 3)
        def _():
            stream(
                steps, buf, sem,
                lambda s: dot_t(tiles(own_ref, s // tall, TILE), tiles(held, lax.rem(s, tall), TILE)),
                lambda s: out_ref.at[0, 1, pl.ds(s // tall * TILE, TILE), pl.ds(first + lax.rem(s, tall) * TILE, TILE)],
            )

    scratch = [pltpu.VMEM((size, depth), jnp.bfloat16), pltpu.SemaphoreType.DMA]
    return call(kernel, size, rows, depth, out, [(part, pl.ANY), (own, pltpu.VMEM)], scratch, (TILE, TILE))


def slot2(first, size, near_first, near, far, own, out):
    rows, depth = own.shape
    high = min(size, TILE)

    def kernel(near_ref, far_ref, own_ref, _, out_ref, buf, sem, held, held_sem):
        p = lax.axis_index("row")
        tall = size // high
        steps = tall * (rows // TILE)

        def place(s):
            return out_ref.at[0, 2, pl.ds(first + lax.rem(s, tall) * high, high), pl.ds(s // tall * TILE, TILE)]

        @pl.when(p == 0)
        def _():
            load = pltpu.make_async_copy(near_ref.at[pl.ds(first - near_first, size), :], held, held_sem)
            load.start()
            load.wait()

        @pl.when(p == 1)
        def _():
            load = pltpu.make_async_copy(far_ref, held, held_sem)
            load.start()
            load.wait()

        @pl.when(p < 2)
        def _():
            stream(steps, buf, sem, lambda s: dot_t(tiles(held, lax.rem(s, tall), high), tiles(own_ref, s // tall, TILE)), place)

        @pl.when(p >= 2)
        def _():
            stream(steps, buf, sem, lambda s: jnp.zeros((high, TILE), jnp.float32), place)

    scratch = [pltpu.VMEM((size, depth), jnp.bfloat16), pltpu.SemaphoreType.DMA]
    refs = [(near, pl.ANY), (far, pl.ANY), (own, pltpu.VMEM)]
    return call(kernel, size, rows, depth, out, refs, scratch, (high, TILE))


def solution(mesh):
    assert mesh.shape["row"] == 4

    def send(a, pairs):
        return lax.ppermute(a, "row", pairs)

    def local(a):
        parts = [send(a[first:first + size], NEXT) for first, size in PARTS]
        out = diag(a)
        passed = [send(part, PASS) for part in parts]
        far = [send(a[first:first + size], FAR) for first, size in FARS]
        for k, (first, size) in enumerate(PARTS):
            out = slot1(first, size, parts[k], a, out)
        for j, (first, size) in enumerate(FARS):
            near = max(k for k, (start, _) in enumerate(PARTS) if start <= first)
            out = slot2(first, size, PARTS[near][0], passed[near], far[j], a, out)
        return out

    return jax.shard_map(
        local, mesh=mesh, in_specs=(P(("mat", "row"), None),), out_specs=P(("mat", "row"), None, None, None), check_vma=False
    )
```

```python
import jax
import jax.numpy as jnp
from jax import lax
from jax.experimental import pallas as pl
from jax.experimental.pallas import tpu as pltpu
from jax.sharding import PartitionSpec as P


TILE = 512
WIDE = 896
NEXT = [(1, 0), (2, 1), (3, 2), (0, 3)]
FAR = [(3, 1)]
PASS = [(1, 0)]
PARTS = [(0, 512), (512, 1536), (2048, 1024), (3072, 512)]
FARS = [(0, 1024), (1024, 1024), (2048, 640), (2688, 448), (3136, 256), (3392, 192)]
DEPTH = 3


def dot_t(x, y):
    return lax.dot_general(x, y, (((1,), (1,)), ((), ())), preferred_element_type=jnp.float32)


def tiles(ref, index, size):
    return ref[pl.ds(pl.multiple_of(index * size, size), size), :]


def stream(steps, buf, sem, value, place):
    def copy(s):
        return pltpu.make_async_copy(buf.at[lax.rem(s, DEPTH)], place(s), sem.at[lax.rem(s, DEPTH)])

    @pl.loop(0, steps)
    def _(s):
        @pl.when(s >= DEPTH)
        def _():
            copy(s - DEPTH).wait()

        buf[lax.rem(s, DEPTH)] = value(s)
        copy(s).start()

    for s in range(max(steps - DEPTH, 0), steps):
        copy(s).wait()


def load(src, dst, sem):
    copy = pltpu.make_async_copy(src, dst, sem)
    copy.start()
    copy.wait()


def call(kernel, rows, cols, depth, out, refs, scratch):
    made = isinstance(out, jax.ShapeDtypeStruct)
    args = [a for a, _ in refs] + ([] if made else [out])
    return pl.pallas_call(
        kernel,
        in_specs=[pl.BlockSpec(memory_space=space) for _, space in refs] + ([] if made else [pl.BlockSpec(memory_space=pl.ANY)]),
        out_specs=pl.BlockSpec(memory_space=pl.ANY),
        out_shape=jax.ShapeDtypeStruct(out.shape, out.dtype),
        input_output_aliases={} if made else {len(args) - 1: 0},
        scratch_shapes=[pltpu.SemaphoreType.DMA((DEPTH,)), pltpu.SemaphoreType.DMA, *scratch],
        cost_estimate=pl.CostEstimate(
            flops=2 * rows * cols * depth, bytes_accessed=4 * rows * cols + 2 * rows * depth, transcendentals=0
        ),
        compiler_params=pltpu.CompilerParams(vmem_limit_bytes=32 << 20),
    )(*args)


def diag(own):
    rows, depth = own.shape
    wide = rows // WIDE

    def kernel(own_ref, out_ref, sem, _, buf):
        stream(
            rows // TILE * wide, buf, sem,
            lambda s: dot_t(tiles(own_ref, s // wide, TILE), tiles(own_ref, lax.rem(s, wide), WIDE)),
            lambda s: out_ref.at[0, 0, pl.ds(s // wide * TILE, TILE), pl.ds(lax.rem(s, wide) * WIDE, WIDE)],
        )

    out = jax.ShapeDtypeStruct((1, 3, rows, rows), jnp.float32)
    scratch = [pltpu.VMEM((DEPTH, TILE, WIDE), jnp.float32)]
    return call(kernel, rows, rows, depth, out, [(own, pltpu.VMEM)], scratch)


def slot1(first, size, part, own, out):
    rows, depth = own.shape
    tall = size // TILE
    steps = tall * (rows // WIDE)

    def kernel(part_ref, own_ref, _, out_ref, sem, load_sem, held, buf, turned):
        p = lax.axis_index("row")
        load(part_ref, held, load_sem)

        @pl.when(p < 3)
        def _():
            stream(
                steps, buf, sem,
                lambda s: dot_t(tiles(held, lax.rem(s, tall), TILE), tiles(own_ref, s // tall, WIDE)),
                lambda s: out_ref.at[0, 1, pl.ds(first + lax.rem(s, tall) * TILE, TILE), pl.ds(s // tall * WIDE, WIDE)],
            )

        @pl.when(p == 3)
        def _():
            stream(
                steps, turned, sem,
                lambda s: dot_t(tiles(own_ref, s // tall, WIDE), tiles(held, lax.rem(s, tall), TILE)),
                lambda s: out_ref.at[0, 1, pl.ds(s // tall * WIDE, WIDE), pl.ds(first + lax.rem(s, tall) * TILE, TILE)],
            )

    scratch = [
        pltpu.VMEM((size, depth), jnp.bfloat16),
        pltpu.VMEM((DEPTH, TILE, WIDE), jnp.float32),
        pltpu.VMEM((DEPTH, WIDE, TILE), jnp.float32),
    ]
    return call(kernel, size, rows, depth, out, [(part, pl.ANY), (own, pltpu.VMEM)], scratch)


def slot2(first, size, passed, far, own, out):
    rows, depth = own.shape
    tall = -(-size // TILE)
    high = size // tall
    wide = WIDE if high > 256 else 2 * WIDE
    steps = tall * (rows // wide)
    near = []
    for (start, count), part in zip(PARTS, passed):
        low, end = max(first, start), min(first + size, start + count)
        if low < end:
            near.append((part, low - start, low - first, end - low))

    def kernel(*refs):
        near_refs, (far_ref, own_ref, _, out_ref, sem, load_sem, held, buf) = refs[:len(near)], refs[len(near):]
        p = lax.axis_index("row")

        def place(s):
            return out_ref.at[0, 2, pl.ds(first + lax.rem(s, tall) * high, high), pl.ds(s // tall * wide, wide)]

        @pl.when(p == 0)
        def _():
            for ref, (_, src, dst, count) in zip(near_refs, near):
                load(ref.at[pl.ds(src, count), :], held.at[pl.ds(dst, count), :], load_sem)

        @pl.when(p == 1)
        def _():
            load(far_ref, held, load_sem)

        @pl.when(p < 2)
        def _():
            stream(steps, buf, sem, lambda s: dot_t(tiles(held, lax.rem(s, tall), high), tiles(own_ref, s // tall, wide)), place)

        @pl.when(p >= 2)
        def _():
            stream(steps, buf, sem, lambda s: jnp.zeros((high, wide), jnp.float32), place)

    scratch = [pltpu.VMEM((size, depth), jnp.bfloat16), pltpu.VMEM((DEPTH, high, wide), jnp.float32)]
    refs = [(part, pl.ANY) for part, *_ in near] + [(far, pl.ANY), (own, pltpu.VMEM)]
    return call(kernel, size, rows, depth, out, refs, scratch)


def solution(mesh):
    assert mesh.shape["row"] == 4

    def send(a, pairs):
        return lax.ppermute(a, "row", pairs)

    def rows_of(a, chunk):
        return a[chunk[0]:chunk[0] + chunk[1]]

    def local(a):
        head = rows_of(a, PARTS[0])
        rest, head = lax.optimization_barrier((a, head))
        parts = [send(head, NEXT)]
        parts += [send(rows_of(rest, PARTS[k]), NEXT) for k in range(1, len(PARTS))]
        out = diag(a)
        passed = [send(part, PASS) for part in parts]
        later, _ = lax.optimization_barrier((a, parts[0]))
        far = [send(rows_of(later, chunk), FAR) for chunk in FARS]
        for k, chunk in enumerate(PARTS):
            out = slot1(*chunk, parts[k], a, out)
        for j, chunk in enumerate(FARS):
            out = slot2(*chunk, passed, far[j], a, out)
        return out

    return jax.shard_map(
        local, mesh=mesh, in_specs=(P(("mat", "row"), None),), out_specs=P(("mat", "row"), None, None, None), check_vma=False
    )
```

```python
import jax
import jax.numpy as jnp
from jax import lax
from jax.experimental import pallas as pl
from jax.experimental.pallas import tpu as pltpu
from jax.sharding import PartitionSpec as P


WIDE = 512
HIGH = 1792
NEXT = [(1, 0), (2, 1), (3, 2), (0, 3)]
FAR = [(3, 1)]
PASS = [(1, 0)]
PARTS = [(0, 512), (512, 1536), (2048, 1024), (3072, 512)]
FARS = [(0, 1024), (1024, 1024), (2048, 640), (2688, 384), (3072, 256), (3328, 256)]
DEPTH = 3
FEW = 384
PIECES = [(0, 1536), (1536, 1536), (3072, 512)]


def dot_t(x, y):
    return lax.dot_general(x, y, (((1,), (1,)), ((), ())), preferred_element_type=jnp.float32)


def tiles(ref, index, size):
    return ref[pl.ds(pl.multiple_of(index * size, size), size), :]


def stream(steps, buf, sem, value, place):
    def copy(s):
        return pltpu.make_async_copy(buf.at[lax.rem(s, DEPTH)], place(s), sem.at[lax.rem(s, DEPTH)])

    @pl.loop(0, steps)
    def _(s):
        @pl.when(s >= DEPTH)
        def _():
            copy(s - DEPTH).wait()

        buf[lax.rem(s, DEPTH)] = value(s)
        copy(s).start()

    for s in range(max(steps - DEPTH, 0), steps):
        copy(s).wait()


def load(src, dst, sem):
    copy = pltpu.make_async_copy(src, dst, sem)
    copy.start()
    copy.wait()


def call(kernel, rows, cols, depth, out, refs, scratch):
    made = isinstance(out, jax.ShapeDtypeStruct)
    args = [a for a, _ in refs] + ([] if made else [out])
    return pl.pallas_call(
        kernel,
        in_specs=[pl.BlockSpec(memory_space=space) for _, space in refs] + ([] if made else [pl.BlockSpec(memory_space=pl.ANY)]),
        out_specs=pl.BlockSpec(memory_space=pl.ANY),
        out_shape=jax.ShapeDtypeStruct(out.shape, out.dtype),
        input_output_aliases={} if made else {len(args) - 1: 0},
        scratch_shapes=[pltpu.SemaphoreType.DMA((DEPTH,)), pltpu.SemaphoreType.DMA, *scratch],
        cost_estimate=pl.CostEstimate(
            flops=2 * rows * cols * depth, bytes_accessed=4 * rows * cols + 2 * rows * depth, transcendentals=0
        ),
        compiler_params=pltpu.CompilerParams(vmem_limit_bytes=32 << 20),
    )(*args)


def diag(own):
    rows, depth = own.shape
    wide = rows // WIDE

    def kernel(own_ref, out_ref, sem, _, buf):
        stream(
            rows // HIGH * wide, buf, sem,
            lambda s: dot_t(tiles(own_ref, s // wide, HIGH), tiles(own_ref, lax.rem(s, wide), WIDE)),
            lambda s: out_ref.at[0, 0, pl.ds(s // wide * HIGH, HIGH), pl.ds(lax.rem(s, wide) * WIDE, WIDE)],
        )

    out = jax.ShapeDtypeStruct((1, 3, rows, rows), jnp.float32)
    return call(kernel, rows, rows, depth, out, [(own, pltpu.VMEM)], [pltpu.VMEM((DEPTH, HIGH, WIDE), jnp.float32)])


def slot1(first, size, part, own, out):
    rows, depth = own.shape
    tall = size // WIDE

    def kernel(part_ref, own_ref, _, out_ref, sem, load_sem, held, buf):
        p = lax.axis_index("row")
        load(part_ref, held, load_sem)

        @pl.when(p < 3)
        def _():
            stream(
                rows // WIDE, buf.at[:, :size], sem,
                lambda s: dot_t(held[...], tiles(own_ref, s, WIDE)),
                lambda s: out_ref.at[0, 1, pl.ds(first, size), pl.ds(s * WIDE, WIDE)],
            )

        @pl.when(p == 3)
        def _():
            stream(
                rows // HIGH * tall, buf, sem,
                lambda s: dot_t(tiles(own_ref, s // tall, HIGH), tiles(held, lax.rem(s, tall), WIDE)),
                lambda s: out_ref.at[0, 1, pl.ds(s // tall * HIGH, HIGH), pl.ds(first + lax.rem(s, tall) * WIDE, WIDE)],
            )

    scratch = [pltpu.VMEM((size, depth), jnp.bfloat16), pltpu.VMEM((DEPTH, HIGH, WIDE), jnp.float32)]
    return call(kernel, size, rows, depth, out, [(part, pl.ANY), (own, pltpu.VMEM)], scratch)


def slot2(first, size, passed, far, own, out):
    rows, depth = own.shape
    near = []
    for (start, count), part in zip(PARTS, passed):
        low, end = max(first, start), min(first + size, start + count)
        if low < end:
            near.append((part, low - start, low - first, end - low))

    def kernel(*refs):
        near_refs, (far_ref, own_ref, _, out_ref, sem, load_sem, held, buf) = refs[:len(near)], refs[len(near):]
        p = lax.axis_index("row")

        def place(start, wide):
            return out_ref.at[0, 2, pl.ds(first, size), pl.ds(start, wide)]

        @pl.when(p == 0)
        def _():
            for ref, (_, src, dst, count) in zip(near_refs, near):
                load(ref.at[pl.ds(src, count), :], held.at[pl.ds(dst, count), :], load_sem)

        @pl.when(p == 1)
        def _():
            load(far_ref, held, load_sem)

        def zeros(wide):
            stream(
                rows // wide, buf.at[:, :, :wide], sem,
                lambda s: jnp.zeros((size, wide), jnp.float32),
                lambda s: place(s * wide, wide),
            )

        if size > FEW:

            @pl.when(p < 2)
            def _():
                stream(
                    rows // WIDE, buf, sem,
                    lambda s: dot_t(held[...], tiles(own_ref, s, WIDE)),
                    lambda s: place(s * WIDE, WIDE),
                )

        else:

            @pl.when(p < 2)
            def _():
                copies = []
                for k, (start, wide) in enumerate(PIECES):
                    buf[k, :, :wide] = dot_t(held[...], own_ref[start:start + wide, :])
                    copies.append(pltpu.make_async_copy(buf.at[k, :, :wide], place(start, wide), sem.at[k]))
                    copies[-1].start()
                for copy in copies:
                    copy.wait()

        @pl.when(p >= 2)
        def _():
            zeros(WIDE)

    width = WIDE if size > FEW else PIECES[0][1]
    scratch = [pltpu.VMEM((size, depth), jnp.bfloat16), pltpu.VMEM((DEPTH, size, width), jnp.float32)]
    refs = [(part, pl.ANY) for part, *_ in near] + [(far, pl.ANY), (own, pltpu.VMEM)]
    return call(kernel, size, rows, depth, out, refs, scratch)


def solution(mesh):
    assert mesh.shape["row"] == 4

    def send(a, pairs):
        return lax.ppermute(a, "row", pairs)

    def rows_of(a, chunk):
        return a[chunk[0]:chunk[0] + chunk[1]]

    def local(a):
        head = rows_of(a, PARTS[0])
        rest, head = lax.optimization_barrier((a, head))
        parts = [send(head, NEXT)]
        parts += [send(rows_of(rest, PARTS[k]), NEXT) for k in range(1, len(PARTS))]
        out = diag(a)
        passed = [send(part, PASS) for part in parts]
        later, _ = lax.optimization_barrier((a, parts[0]))
        far = [send(rows_of(later, chunk), FAR) for chunk in FARS]
        for k, chunk in enumerate(PARTS):
            out = slot1(*chunk, parts[k], a, out)
        for j, chunk in enumerate(FARS):
            out = slot2(*chunk, passed, far[j], a, out)
        return out

    return jax.shard_map(
        local, mesh=mesh, in_specs=(P(("mat", "row"), None),), out_specs=P(("mat", "row"), None, None, None), check_vma=False
    )
```

```python
import jax
import jax.numpy as jnp
from jax import lax
from jax.experimental import pallas as pl
from jax.experimental.pallas import tpu as pltpu
from jax.sharding import PartitionSpec as P


WIDE = 512
HIGH = 1792
NEXT = [(1, 0), (2, 1), (3, 2), (0, 3)]
FAR = [(3, 1)]
PASS = [(1, 0)]
PARTS = [(0, 256), (256, 1792), (2048, 1024), (3072, 512)]
FARS = [(0, 1024), (1024, 1024), (2048, 640), (2688, 384), (3072, 256), (3328, 256)]
DEPTH = 3
FEW = 384
PIECES = [(0, 1536), (1536, 1536), (3072, 512)]


def dot_t(x, y):
    return lax.dot_general(x, y, (((1,), (1,)), ((), ())), preferred_element_type=jnp.float32)


def tiles(ref, index, size):
    return ref[pl.ds(pl.multiple_of(index * size, size), size), :]


def stream(steps, buf, sem, value, place):
    def copy(s):
        return pltpu.make_async_copy(buf.at[lax.rem(s, DEPTH)], place(s), sem.at[lax.rem(s, DEPTH)])

    @pl.loop(0, steps)
    def _(s):
        @pl.when(s >= DEPTH)
        def _():
            copy(s - DEPTH).wait()

        buf[lax.rem(s, DEPTH)] = value(s)
        copy(s).start()

    for s in range(max(steps - DEPTH, 0), steps):
        copy(s).wait()


def load(src, dst, sem):
    copy = pltpu.make_async_copy(src, dst, sem)
    copy.start()
    copy.wait()


def call(kernel, rows, cols, depth, out, refs, scratch):
    made = isinstance(out, jax.ShapeDtypeStruct)
    args = [a for a, _ in refs] + ([] if made else [out])
    return pl.pallas_call(
        kernel,
        in_specs=[pl.BlockSpec(memory_space=space) for _, space in refs] + ([] if made else [pl.BlockSpec(memory_space=pl.ANY)]),
        out_specs=pl.BlockSpec(memory_space=pl.ANY),
        out_shape=jax.ShapeDtypeStruct(out.shape, out.dtype),
        input_output_aliases={} if made else {len(args) - 1: 0},
        scratch_shapes=[pltpu.SemaphoreType.DMA((DEPTH,)), pltpu.SemaphoreType.DMA, *scratch],
        cost_estimate=pl.CostEstimate(
            flops=2 * rows * cols * depth, bytes_accessed=4 * rows * cols + 2 * rows * depth, transcendentals=0
        ),
        compiler_params=pltpu.CompilerParams(vmem_limit_bytes=32 << 20),
    )(*args)


def bring(a):
    def kernel(a_ref, own_ref, sem):
        load(a_ref, own_ref, sem)

    return pl.pallas_call(
        kernel,
        in_specs=[pl.BlockSpec(memory_space=pl.ANY)],
        out_specs=pl.BlockSpec(memory_space=pltpu.VMEM),
        out_shape=pltpu.VMEM(a.shape, a.dtype),
        scratch_shapes=[pltpu.SemaphoreType.DMA],
        cost_estimate=pl.CostEstimate(flops=0, bytes_accessed=4 * a.size, transcendentals=0),
        compiler_params=pltpu.CompilerParams(vmem_limit_bytes=51 << 20),
        name="bring",
    )(a)


def diag(own):
    rows, depth = own.shape
    wide = rows // WIDE

    def kernel(own_ref, out_ref, sem, _, buf):
        stream(
            rows // HIGH * wide, buf, sem,
            lambda s: dot_t(tiles(own_ref, s // wide, HIGH), tiles(own_ref, lax.rem(s, wide), WIDE)),
            lambda s: out_ref.at[0, 0, pl.ds(s // wide * HIGH, HIGH), pl.ds(lax.rem(s, wide) * WIDE, WIDE)],
        )

    out = jax.ShapeDtypeStruct((1, 3, rows, rows), jnp.float32)
    return call(kernel, rows, rows, depth, out, [(own, pltpu.VMEM)], [pltpu.VMEM((DEPTH, HIGH, WIDE), jnp.float32)])


def slot1(first, size, part, own, out):
    rows, depth = own.shape
    wide = WIDE if size % WIDE == 0 else WIDE // 2
    tall = size // wide

    def kernel(part_ref, own_ref, _, out_ref, sem, load_sem, held, buf):
        p = lax.axis_index("row")
        load(part_ref, held, load_sem)

        @pl.when(p < 3)
        def _():
            stream(
                rows // WIDE, buf.at[:, :size], sem,
                lambda s: dot_t(held[...], tiles(own_ref, s, WIDE)),
                lambda s: out_ref.at[0, 1, pl.ds(first, size), pl.ds(s * WIDE, WIDE)],
            )

        @pl.when(p == 3)
        def _():
            stream(
                rows // HIGH * tall, buf.at[:, :, :wide], sem,
                lambda s: dot_t(tiles(own_ref, s // tall, HIGH), tiles(held, lax.rem(s, tall), wide)),
                lambda s: out_ref.at[0, 1, pl.ds(s // tall * HIGH, HIGH), pl.ds(first + lax.rem(s, tall) * wide, wide)],
            )

    scratch = [pltpu.VMEM((size, depth), jnp.bfloat16), pltpu.VMEM((DEPTH, HIGH, WIDE), jnp.float32)]
    return call(kernel, size, rows, depth, out, [(part, pl.ANY), (own, pltpu.VMEM)], scratch)


def slot2(first, size, passed, far, own, out):
    rows, depth = own.shape
    near = []
    for (start, count), part in zip(PARTS, passed):
        low, end = max(first, start), min(first + size, start + count)
        if low < end:
            near.append((part, low - start, low - first, end - low))

    def kernel(*refs):
        near_refs, (far_ref, own_ref, _, out_ref, sem, load_sem, held, buf) = refs[:len(near)], refs[len(near):]
        p = lax.axis_index("row")

        def place(start, wide):
            return out_ref.at[0, 2, pl.ds(first, size), pl.ds(start, wide)]

        @pl.when(p == 0)
        def _():
            for ref, (_, src, dst, count) in zip(near_refs, near):
                load(ref.at[pl.ds(src, count), :], held.at[pl.ds(dst, count), :], load_sem)

        @pl.when(p == 1)
        def _():
            load(far_ref, held, load_sem)

        def zeros(wide):
            stream(
                rows // wide, buf.at[:, :, :wide], sem,
                lambda s: jnp.zeros((size, wide), jnp.float32),
                lambda s: place(s * wide, wide),
            )

        if size > FEW:

            @pl.when(p < 2)
            def _():
                stream(
                    rows // WIDE, buf, sem,
                    lambda s: dot_t(held[...], tiles(own_ref, s, WIDE)),
                    lambda s: place(s * WIDE, WIDE),
                )

        else:

            @pl.when(p < 2)
            def _():
                copies = []
                for k, (start, wide) in enumerate(PIECES):
                    buf[k, :, :wide] = dot_t(held[...], own_ref[start:start + wide, :])
                    copies.append(pltpu.make_async_copy(buf.at[k, :, :wide], place(start, wide), sem.at[k]))
                    copies[-1].start()
                for copy in copies:
                    copy.wait()

        @pl.when(p >= 2)
        def _():
            zeros(WIDE)

    width = WIDE if size > FEW else PIECES[0][1]
    scratch = [pltpu.VMEM((size, depth), jnp.bfloat16), pltpu.VMEM((DEPTH, size, width), jnp.float32)]
    refs = [(part, pl.ANY) for part, *_ in near] + [(far, pl.ANY), (own, pltpu.VMEM)]
    return call(kernel, size, rows, depth, out, refs, scratch)


def solution(mesh):
    assert mesh.shape["row"] == 4

    def send(a, pairs):
        return lax.ppermute(a, "row", pairs)

    def rows_of(a, chunk):
        return a[chunk[0]:chunk[0] + chunk[1]]

    def local(a):
        head = rows_of(a, PARTS[0])
        parts = [send(head, NEXT)]
        own = bring(a)
        parts += [send(rows_of(own, PARTS[k]), NEXT) for k in range(1, len(PARTS))]
        out = diag(own)
        passed = [send(part, PASS) for part in parts]
        later, _ = lax.optimization_barrier((own, parts[0]))
        far = [send(rows_of(later, chunk), FAR) for chunk in FARS]
        for k, chunk in enumerate(PARTS):
            out = slot1(*chunk, parts[k], own, out)
        for j, chunk in enumerate(FARS):
            out = slot2(*chunk, passed, far[j], own, out)
        return out

    return jax.shard_map(
        local, mesh=mesh, in_specs=(P(("mat", "row"), None),), out_specs=P(("mat", "row"), None, None, None), check_vma=False
    )
```

```python
import jax
import jax.numpy as jnp
from jax import lax
from jax.experimental import pallas as pl
from jax.experimental.pallas import tpu as pltpu
from jax.sharding import PartitionSpec as P


WIDE = 512
HIGH = 1792
NEXT = [(1, 0), (2, 1), (3, 2), (0, 3)]
FAR = [(3, 1)]
PASS = [(1, 0)]
PARTS = [(0, 256), (256, 1792), (2048, 1024), (3072, 512)]
FARS = [(0, 1024), (1024, 848), (1872, 640), (2512, 416), (2928, 272), (3200, 208), (3408, 176)]
TURN_AFTER = 0
DEPTH = 3
FEW = 448
PIECES = [(0, 2560), (2560, 1024)]


def dot_t(x, y):
    return lax.dot_general(x, y, (((1,), (1,)), ((), ())), preferred_element_type=jnp.float32)


def tiles(ref, index, size):
    return ref[pl.ds(pl.multiple_of(index * size, size), size), :]


def stream(steps, buf, sem, value, place):
    def copy(s):
        return pltpu.make_async_copy(buf.at[lax.rem(s, DEPTH)], place(s), sem.at[lax.rem(s, DEPTH)])

    @pl.loop(0, steps)
    def _(s):
        @pl.when(s >= DEPTH)
        def _():
            copy(s - DEPTH).wait()

        buf[lax.rem(s, DEPTH)] = value(s)
        copy(s).start()

    for s in range(max(steps - DEPTH, 0), steps):
        copy(s).wait()


def load(src, dst, sem):
    copy = pltpu.make_async_copy(src, dst, sem)
    copy.start()
    copy.wait()


def call(kernel, rows, cols, depth, out, refs, scratch):
    made = isinstance(out, jax.ShapeDtypeStruct)
    args = [a for a, _ in refs] + ([] if made else [out])
    return pl.pallas_call(
        kernel,
        in_specs=[pl.BlockSpec(memory_space=space) for _, space in refs] + ([] if made else [pl.BlockSpec(memory_space=pl.ANY)]),
        out_specs=pl.BlockSpec(memory_space=pl.ANY),
        out_shape=jax.ShapeDtypeStruct(out.shape, out.dtype),
        input_output_aliases={} if made else {len(args) - 1: 0},
        scratch_shapes=[pltpu.SemaphoreType.DMA((DEPTH,)), pltpu.SemaphoreType.DMA, *scratch],
        cost_estimate=pl.CostEstimate(
            flops=2 * rows * cols * depth, bytes_accessed=4 * rows * cols + 2 * rows * depth, transcendentals=0
        ),
        compiler_params=pltpu.CompilerParams(vmem_limit_bytes=32 << 20),
    )(*args)


def bring(a):
    def kernel(a_ref, own_ref, sem):
        load(a_ref, own_ref, sem)

    return pl.pallas_call(
        kernel,
        in_specs=[pl.BlockSpec(memory_space=pl.ANY)],
        out_specs=pl.BlockSpec(memory_space=pltpu.VMEM),
        out_shape=pltpu.VMEM(a.shape, a.dtype),
        scratch_shapes=[pltpu.SemaphoreType.DMA],
        cost_estimate=pl.CostEstimate(flops=0, bytes_accessed=4 * a.size, transcendentals=0),
        compiler_params=pltpu.CompilerParams(vmem_limit_bytes=51 << 20),
        name="bring",
    )(a)


def turn(own, out):
    rows, depth = own.shape

    def kernel(own_ref, _, turned_ref, out_ref):
        @pl.when(lax.axis_index("row") < 2)
        def _():
            @pl.loop(0, rows // WIDE)
            def _(s):
                turned_ref[:, pl.ds(pl.multiple_of(s * WIDE, WIDE), WIDE)] = tiles(own_ref, s, WIDE).T

    return pl.pallas_call(
        kernel,
        in_specs=[pl.BlockSpec(memory_space=pltpu.VMEM), pl.BlockSpec(memory_space=pl.ANY)],
        out_specs=[pl.BlockSpec(memory_space=pltpu.VMEM), pl.BlockSpec(memory_space=pl.ANY)],
        out_shape=[pltpu.VMEM((depth, rows), own.dtype), jax.ShapeDtypeStruct(out.shape, out.dtype)],
        input_output_aliases={1: 1},
        cost_estimate=pl.CostEstimate(flops=0, bytes_accessed=4 * own.size, transcendentals=0),
        compiler_params=pltpu.CompilerParams(vmem_limit_bytes=32 << 20),
        name="turn",
    )(own, out)


def diag(own):
    rows, depth = own.shape
    wide = rows // WIDE

    def kernel(own_ref, out_ref, sem, _, buf):
        stream(
            rows // HIGH * wide, buf, sem,
            lambda s: dot_t(tiles(own_ref, s // wide, HIGH), tiles(own_ref, lax.rem(s, wide), WIDE)),
            lambda s: out_ref.at[0, 0, pl.ds(s // wide * HIGH, HIGH), pl.ds(lax.rem(s, wide) * WIDE, WIDE)],
        )

    out = jax.ShapeDtypeStruct((1, 3, rows, rows), jnp.float32)
    return call(kernel, rows, rows, depth, out, [(own, pltpu.VMEM)], [pltpu.VMEM((DEPTH, HIGH, WIDE), jnp.float32)])


def slot1(first, size, part, own, out):
    rows, depth = own.shape
    wide = WIDE if size % WIDE == 0 else WIDE // 2
    tall = size // wide

    def kernel(part_ref, own_ref, _, out_ref, sem, load_sem, held, buf):
        p = lax.axis_index("row")
        load(part_ref, held, load_sem)

        @pl.when(p < 3)
        def _():
            stream(
                rows // WIDE, buf.at[:, :size], sem,
                lambda s: dot_t(held[...], tiles(own_ref, s, WIDE)),
                lambda s: out_ref.at[0, 1, pl.ds(first, size), pl.ds(s * WIDE, WIDE)],
            )

        @pl.when(p == 3)
        def _():
            stream(
                rows // HIGH * tall, buf.at[:, :, :wide], sem,
                lambda s: dot_t(tiles(own_ref, s // tall, HIGH), tiles(held, lax.rem(s, tall), wide)),
                lambda s: out_ref.at[0, 1, pl.ds(s // tall * HIGH, HIGH), pl.ds(first + lax.rem(s, tall) * wide, wide)],
            )

    scratch = [pltpu.VMEM((size, depth), jnp.bfloat16), pltpu.VMEM((DEPTH, HIGH, WIDE), jnp.float32)]
    return call(kernel, size, rows, depth, out, [(part, pl.ANY), (own, pltpu.VMEM)], scratch)


def slot2(first, size, passed, far, own, out):
    rows, depth = own.shape if size > FEW else own.shape[::-1]
    near = []
    for (start, count), part in zip(PARTS, passed):
        low, end = max(first, start), min(first + size, start + count)
        if low < end:
            near.append((part, low - start, low - first, end - low))

    def kernel(*refs):
        near_refs, (far_ref, own_ref, _, out_ref, sem, load_sem, held, buf) = refs[:len(near)], refs[len(near):]
        p = lax.axis_index("row")

        def place(start, wide):
            return out_ref.at[0, 2, pl.ds(first, size), pl.ds(start, wide)]

        @pl.when(p == 0)
        def _():
            for ref, (_, src, dst, count) in zip(near_refs, near):
                load(ref.at[pl.ds(src, count), :], held.at[pl.ds(dst, count), :], load_sem)

        @pl.when(p == 1)
        def _():
            load(far_ref, held, load_sem)

        def zeros(wide):
            stream(
                rows // wide, buf.at[:, :, :wide], sem,
                lambda s: jnp.zeros((size, wide), jnp.float32),
                lambda s: place(s * wide, wide),
            )

        if size > FEW:

            @pl.when(p < 2)
            def _():
                stream(
                    rows // WIDE, buf, sem,
                    lambda s: dot_t(held[...], tiles(own_ref, s, WIDE)),
                    lambda s: place(s * WIDE, WIDE),
                )

        else:

            @pl.when(p < 2)
            def _():
                copies = []
                for k, (start, wide) in enumerate(PIECES):
                    buf[k, :, :wide] = jnp.dot(held[...], own_ref[:, start:start + wide], preferred_element_type=jnp.float32)
                    copies.append(pltpu.make_async_copy(buf.at[k, :, :wide], place(start, wide), sem.at[k]))
                    copies[-1].start()
                for copy in copies:
                    copy.wait()

        @pl.when(p >= 2)
        def _():
            zeros(WIDE)

    width = WIDE if size > FEW else PIECES[0][1]
    scratch = [pltpu.VMEM((size, depth), jnp.bfloat16), pltpu.VMEM((DEPTH, size, width), jnp.float32)]
    refs = [(part, pl.ANY) for part, *_ in near] + [(far, pl.ANY), (own, pltpu.VMEM)]
    return call(kernel, size, rows, depth, out, refs, scratch)


def solution(mesh):
    assert mesh.shape["row"] == 4

    def send(a, pairs):
        return lax.ppermute(a, "row", pairs)

    def rows_of(a, chunk):
        return a[chunk[0]:chunk[0] + chunk[1]]

    def local(a):
        head = rows_of(a, PARTS[0])
        parts = [send(head, NEXT)]
        own = bring(a)
        parts += [send(rows_of(own, PARTS[k]), NEXT) for k in range(1, len(PARTS))]
        out = diag(own)
        passed = [send(part, PASS) for part in parts]
        later, _ = lax.optimization_barrier((own, parts[0]))
        far = [send(rows_of(later, chunk), FAR) for chunk in FARS]
        for k, chunk in enumerate(PARTS):
            out = slot1(*chunk, parts[k], own, out)
        for j, chunk in enumerate(FARS):
            out = slot2(*chunk, passed, far[j], own if chunk[1] > FEW else turned, out)
            if j == TURN_AFTER:
                turned, out = turn(own, out)
        return out

    return jax.shard_map(
        local, mesh=mesh, in_specs=(P(("mat", "row"), None),), out_specs=P(("mat", "row"), None, None, None), check_vma=False
    )
```

```python
import jax
import jax.numpy as jnp
from jax import lax
from jax.experimental import pallas as pl
from jax.experimental.pallas import tpu as pltpu
from jax.sharding import PartitionSpec as P


WIDE = 512
HIGH = 1792
NEXT = [(1, 0), (2, 1), (3, 2), (0, 3)]
FAR = [(3, 1)]
PASS = [(1, 0)]
PARTS = [(0, 256), (256, 1792), (2048, 1024), (3072, 512)]
FARS = [(0, 1024), (1024, 848), (1872, 640), (2512, 416), (2928, 272), (3200, 208), (3408, 176)]
TURN_AFTER = 0
DEPTH = 3
FEW = 448


def dot_t(x, y):
    return lax.dot_general(x, y, (((1,), (1,)), ((), ())), preferred_element_type=jnp.float32)


def tiles(ref, index, size):
    return ref[pl.ds(pl.multiple_of(index * size, size), size), :]


def stream(steps, buf, sem, value, place):
    def copy(s):
        return pltpu.make_async_copy(buf.at[lax.rem(s, DEPTH)], place(s), sem.at[lax.rem(s, DEPTH)])

    @pl.loop(0, steps)
    def _(s):
        @pl.when(s >= DEPTH)
        def _():
            copy(s - DEPTH).wait()

        buf[lax.rem(s, DEPTH)] = value(s)
        copy(s).start()

    for s in range(max(steps - DEPTH, 0), steps):
        copy(s).wait()


def load(src, dst, sem):
    copy = pltpu.make_async_copy(src, dst, sem)
    copy.start()
    copy.wait()


def call(kernel, rows, cols, depth, out, refs, scratch):
    made = isinstance(out, jax.ShapeDtypeStruct)
    args = [a for a, _ in refs] + ([] if made else [out])
    return pl.pallas_call(
        kernel,
        in_specs=[pl.BlockSpec(memory_space=space) for _, space in refs] + ([] if made else [pl.BlockSpec(memory_space=pl.ANY)]),
        out_specs=pl.BlockSpec(memory_space=pl.ANY),
        out_shape=jax.ShapeDtypeStruct(out.shape, out.dtype),
        input_output_aliases={} if made else {len(args) - 1: 0},
        scratch_shapes=[pltpu.SemaphoreType.DMA((8,)), pltpu.SemaphoreType.DMA, *scratch],
        cost_estimate=pl.CostEstimate(
            flops=2 * rows * cols * depth, bytes_accessed=4 * rows * cols + 2 * rows * depth, transcendentals=0
        ),
        compiler_params=pltpu.CompilerParams(vmem_limit_bytes=32 << 20),
    )(*args)


def bring(a):
    def kernel(a_ref, own_ref, sem):
        load(a_ref, own_ref, sem)

    return pl.pallas_call(
        kernel,
        in_specs=[pl.BlockSpec(memory_space=pl.ANY)],
        out_specs=pl.BlockSpec(memory_space=pltpu.VMEM),
        out_shape=pltpu.VMEM(a.shape, a.dtype),
        scratch_shapes=[pltpu.SemaphoreType.DMA],
        cost_estimate=pl.CostEstimate(flops=0, bytes_accessed=4 * a.size, transcendentals=0),
        compiler_params=pltpu.CompilerParams(vmem_limit_bytes=51 << 20),
        name="bring",
    )(a)


def turn(own, out):
    rows, depth = own.shape

    def kernel(own_ref, _, turned_ref, out_ref):
        @pl.when(lax.axis_index("row") < 2)
        def _():
            @pl.loop(0, rows // WIDE)
            def _(s):
                turned_ref[:, pl.ds(pl.multiple_of(s * WIDE, WIDE), WIDE)] = tiles(own_ref, s, WIDE).T

    return pl.pallas_call(
        kernel,
        in_specs=[pl.BlockSpec(memory_space=pltpu.VMEM), pl.BlockSpec(memory_space=pl.ANY)],
        out_specs=[pl.BlockSpec(memory_space=pltpu.VMEM), pl.BlockSpec(memory_space=pl.ANY)],
        out_shape=[pltpu.VMEM((depth, rows), own.dtype), jax.ShapeDtypeStruct(out.shape, out.dtype)],
        input_output_aliases={1: 1},
        cost_estimate=pl.CostEstimate(flops=0, bytes_accessed=4 * own.size, transcendentals=0),
        compiler_params=pltpu.CompilerParams(vmem_limit_bytes=32 << 20),
        name="turn",
    )(own, out)


def diag(own):
    rows, depth = own.shape
    wide = rows // WIDE

    def kernel(own_ref, out_ref, sem, _, buf):
        stream(
            rows // HIGH * wide, buf, sem,
            lambda s: dot_t(tiles(own_ref, s // wide, HIGH), tiles(own_ref, lax.rem(s, wide), WIDE)),
            lambda s: out_ref.at[0, 0, pl.ds(s // wide * HIGH, HIGH), pl.ds(lax.rem(s, wide) * WIDE, WIDE)],
        )

    out = jax.ShapeDtypeStruct((1, 3, rows, rows), jnp.float32)
    return call(kernel, rows, rows, depth, out, [(own, pltpu.VMEM)], [pltpu.VMEM((DEPTH, HIGH, WIDE), jnp.float32)])


def slot1(first, size, part, own, out):
    rows, depth = own.shape
    wide = WIDE if size % WIDE == 0 else WIDE // 2
    tall = size // wide

    def kernel(part_ref, own_ref, _, out_ref, sem, load_sem, held, buf):
        p = lax.axis_index("row")
        load(part_ref, held, load_sem)

        @pl.when(p < 3)
        def _():
            stream(
                rows // WIDE, buf.at[:, :size], sem,
                lambda s: dot_t(held[...], tiles(own_ref, s, WIDE)),
                lambda s: out_ref.at[0, 1, pl.ds(first, size), pl.ds(s * WIDE, WIDE)],
            )

        @pl.when(p == 3)
        def _():
            stream(
                rows // HIGH * tall, buf.at[:, :, :wide], sem,
                lambda s: dot_t(tiles(own_ref, s // tall, HIGH), tiles(held, lax.rem(s, tall), wide)),
                lambda s: out_ref.at[0, 1, pl.ds(s // tall * HIGH, HIGH), pl.ds(first + lax.rem(s, tall) * wide, wide)],
            )

    scratch = [pltpu.VMEM((size, depth), jnp.bfloat16), pltpu.VMEM((DEPTH, HIGH, WIDE), jnp.float32)]
    return call(kernel, size, rows, depth, out, [(part, pl.ANY), (own, pltpu.VMEM)], scratch)


def slot2(first, size, passed, far, own, out):
    rows, depth = own.shape if size > FEW else own.shape[::-1]
    near = []
    for (start, count), part in zip(PARTS, passed):
        low, end = max(first, start), min(first + size, start + count)
        if low < end:
            near.append((part, low - start, low - first, end - low))

    def kernel(*refs):
        near_refs, (far_ref, own_ref, _, out_ref, sem, load_sem, held, buf) = refs[:len(near)], refs[len(near):]
        p = lax.axis_index("row")

        def place(start, wide):
            return out_ref.at[0, 2, pl.ds(first, size), pl.ds(start, wide)]

        @pl.when(p == 0)
        def _():
            for ref, (_, src, dst, count) in zip(near_refs, near):
                load(ref.at[pl.ds(src, count), :], held.at[pl.ds(dst, count), :], load_sem)

        @pl.when(p == 1)
        def _():
            load(far_ref, held, load_sem)

        if size > FEW:

            @pl.when(p < 2)
            def _():
                stream(
                    rows // WIDE, buf, sem,
                    lambda s: dot_t(held[...], tiles(own_ref, s, WIDE)),
                    lambda s: place(s * WIDE, WIDE),
                )

        else:

            @pl.when(p < 2)
            def _():
                copies = []
                for k in range(rows // WIDE):
                    at = slice(k * WIDE, (k + 1) * WIDE)
                    buf[k] = jnp.dot(held[...], own_ref[:, at], preferred_element_type=jnp.float32)
                    copies.append(pltpu.make_async_copy(buf.at[k], place(k * WIDE, WIDE), sem.at[k]))
                    copies[-1].start()
                for copy in copies:
                    copy.wait()

        @pl.when(p >= 2)
        def _():
            stream(
                rows // WIDE, buf, sem,
                lambda s: jnp.zeros((size, WIDE), jnp.float32),
                lambda s: place(s * WIDE, WIDE),
            )

    bufs = DEPTH if size > FEW else rows // WIDE
    scratch = [pltpu.VMEM((size, depth), jnp.bfloat16), pltpu.VMEM((bufs, size, WIDE), jnp.float32)]
    refs = [(part, pl.ANY) for part, *_ in near] + [(far, pl.ANY), (own, pltpu.VMEM)]
    return call(kernel, size, rows, depth, out, refs, scratch)


def solution(mesh):
    assert mesh.shape["row"] == 4

    def send(a, pairs):
        return lax.ppermute(a, "row", pairs)

    def rows_of(a, chunk):
        return a[chunk[0]:chunk[0] + chunk[1]]

    def local(a):
        head = rows_of(a, PARTS[0])
        parts = [send(head, NEXT)]
        own = bring(a)
        parts += [send(rows_of(own, PARTS[k]), NEXT) for k in range(1, len(PARTS))]
        out = diag(own)
        passed = [send(part, PASS) for part in parts]
        later, _ = lax.optimization_barrier((own, parts[0]))
        far = [send(rows_of(later, chunk), FAR) for chunk in FARS]
        for k, chunk in enumerate(PARTS):
            out = slot1(*chunk, parts[k], own, out)
        for j, chunk in enumerate(FARS):
            out = slot2(*chunk, passed, far[j], own if chunk[1] > FEW else turned, out)
            if j == TURN_AFTER:
                turned, out = turn(own, out)
        return out

    return jax.shard_map(
        local, mesh=mesh, in_specs=(P(("mat", "row"), None),), out_specs=P(("mat", "row"), None, None, None), check_vma=False
    )
```

```python
import jax
import jax.numpy as jnp
from jax import lax
from jax.experimental import pallas as pl
from jax.experimental.pallas import tpu as pltpu
from jax.sharding import PartitionSpec as P


WIDE = 512
HIGH = 1792
NEXT = [(1, 0), (2, 1), (3, 2), (0, 3)]
FAR = [(3, 1)]
PASS = [(1, 0)]
PARTS = [(0, 256), (256, 1792), (2048, 1024), (3072, 512)]
FARS = [(0, 816), (816, 768), (1584, 768), (2352, 464), (2816, 272), (3088, 192), (3280, 160), (3440, 144)]
TURN_AFTER = 0
DEPTH = 3
FEW = 464


def dot_t(x, y):
    return lax.dot_general(x, y, (((1,), (1,)), ((), ())), preferred_element_type=jnp.float32)


def tiles(ref, index, size):
    return ref[pl.ds(pl.multiple_of(index * size, size), size), :]


def stream(steps, buf, sem, value, place):
    def copy(s):
        return pltpu.make_async_copy(buf.at[lax.rem(s, DEPTH)], place(s), sem.at[lax.rem(s, DEPTH)])

    @pl.loop(0, steps)
    def _(s):
        @pl.when(s >= DEPTH)
        def _():
            copy(s - DEPTH).wait()

        buf[lax.rem(s, DEPTH)] = value(s)
        copy(s).start()

    for s in range(max(steps - DEPTH, 0), steps):
        copy(s).wait()


def load(src, dst, sem):
    copy = pltpu.make_async_copy(src, dst, sem)
    copy.start()
    copy.wait()


def call(kernel, rows, cols, depth, out, refs, scratch):
    made = isinstance(out, jax.ShapeDtypeStruct)
    args = [a for a, _ in refs] + ([] if made else [out])
    return pl.pallas_call(
        kernel,
        in_specs=[pl.BlockSpec(memory_space=space) for _, space in refs] + ([] if made else [pl.BlockSpec(memory_space=pl.ANY)]),
        out_specs=pl.BlockSpec(memory_space=pl.ANY),
        out_shape=jax.ShapeDtypeStruct(out.shape, out.dtype),
        input_output_aliases={} if made else {len(args) - 1: 0},
        scratch_shapes=[pltpu.SemaphoreType.DMA((8,)), pltpu.SemaphoreType.DMA, *scratch],
        cost_estimate=pl.CostEstimate(
            flops=2 * rows * cols * depth, bytes_accessed=4 * rows * cols + 2 * rows * depth, transcendentals=0
        ),
        compiler_params=pltpu.CompilerParams(vmem_limit_bytes=32 << 20),
    )(*args)


def bring(a, first, size, grant):
    def kernel(a_ref, rows_ref, sem):
        load(a_ref.at[pl.ds(first, size), :], rows_ref, sem)

    return pl.pallas_call(
        kernel,
        in_specs=[pl.BlockSpec(memory_space=pl.ANY)],
        out_specs=pl.BlockSpec(memory_space=pltpu.VMEM),
        out_shape=pltpu.VMEM((size, a.shape[1]), a.dtype),
        scratch_shapes=[pltpu.SemaphoreType.DMA],
        cost_estimate=pl.CostEstimate(flops=0, bytes_accessed=4 * size * a.shape[1], transcendentals=0),
        compiler_params=pltpu.CompilerParams(vmem_limit_bytes=grant),
        name="bring",
    )(a)


def cut(own):
    depth = own.shape[1]

    def kernel(own_ref, *refs):
        piece_refs, sem = refs[:-1], refs[-1]

        @pl.when(lax.axis_index("row") == FAR[0][0])
        def _():
            copies = [
                pltpu.make_async_copy(own_ref.at[pl.ds(first, size), :], piece_ref, sem.at[k])
                for k, ((first, size), piece_ref) in enumerate(zip(FARS, piece_refs))
            ]
            for copy in copies:
                copy.start()
            for copy in copies:
                copy.wait()

    return pl.pallas_call(
        kernel,
        in_specs=[pl.BlockSpec(memory_space=pltpu.VMEM)],
        out_specs=[pl.BlockSpec(memory_space=pl.ANY)] * len(FARS),
        out_shape=[jax.ShapeDtypeStruct((size, depth), own.dtype) for _, size in FARS],
        scratch_shapes=[pltpu.SemaphoreType.DMA((len(FARS),))],
        cost_estimate=pl.CostEstimate(flops=0, bytes_accessed=4 * own.size, transcendentals=0),
        compiler_params=pltpu.CompilerParams(vmem_limit_bytes=32 << 20),
        name="cut",
    )(own)


def turn(own, out):
    rows, depth = own.shape

    def kernel(own_ref, _, turned_ref, out_ref):
        @pl.when(lax.axis_index("row") < 2)
        def _():
            @pl.loop(0, rows // WIDE)
            def _(s):
                turned_ref[:, pl.ds(pl.multiple_of(s * WIDE, WIDE), WIDE)] = tiles(own_ref, s, WIDE).T

    return pl.pallas_call(
        kernel,
        in_specs=[pl.BlockSpec(memory_space=pltpu.VMEM), pl.BlockSpec(memory_space=pl.ANY)],
        out_specs=[pl.BlockSpec(memory_space=pltpu.VMEM), pl.BlockSpec(memory_space=pl.ANY)],
        out_shape=[pltpu.VMEM((depth, rows), own.dtype), jax.ShapeDtypeStruct(out.shape, out.dtype)],
        input_output_aliases={1: 1},
        cost_estimate=pl.CostEstimate(flops=0, bytes_accessed=4 * own.size, transcendentals=0),
        compiler_params=pltpu.CompilerParams(vmem_limit_bytes=32 << 20),
        name="turn",
    )(own, out)


def diag(own):
    rows, depth = own.shape
    wide = rows // WIDE

    def kernel(own_ref, out_ref, sem, _, buf):
        stream(
            rows // HIGH * wide, buf, sem,
            lambda s: dot_t(tiles(own_ref, s // wide, HIGH), tiles(own_ref, lax.rem(s, wide), WIDE)),
            lambda s: out_ref.at[0, 0, pl.ds(s // wide * HIGH, HIGH), pl.ds(lax.rem(s, wide) * WIDE, WIDE)],
        )

    out = jax.ShapeDtypeStruct((1, 3, rows, rows), jnp.float32)
    return call(kernel, rows, rows, depth, out, [(own, pltpu.VMEM)], [pltpu.VMEM((DEPTH, HIGH, WIDE), jnp.float32)])


def slot1(first, size, part, own, out):
    rows, depth = own.shape
    wide = WIDE if size % WIDE == 0 else WIDE // 2
    tall = size // wide

    def kernel(part_ref, own_ref, _, out_ref, sem, load_sem, held, buf):
        p = lax.axis_index("row")
        load(part_ref, held, load_sem)

        @pl.when(p < 3)
        def _():
            stream(
                rows // WIDE, buf.at[:, :size], sem,
                lambda s: dot_t(held[...], tiles(own_ref, s, WIDE)),
                lambda s: out_ref.at[0, 1, pl.ds(first, size), pl.ds(s * WIDE, WIDE)],
            )

        @pl.when(p == 3)
        def _():
            stream(
                rows // HIGH * tall, buf.at[:, :, :wide], sem,
                lambda s: dot_t(tiles(own_ref, s // tall, HIGH), tiles(held, lax.rem(s, tall), wide)),
                lambda s: out_ref.at[0, 1, pl.ds(s // tall * HIGH, HIGH), pl.ds(first + lax.rem(s, tall) * wide, wide)],
            )

    scratch = [pltpu.VMEM((size, depth), jnp.bfloat16), pltpu.VMEM((DEPTH, HIGH, WIDE), jnp.float32)]
    return call(kernel, size, rows, depth, out, [(part, pl.ANY), (own, pltpu.VMEM)], scratch)


def slot2(first, size, passed, far, own, out):
    rows, depth = own.shape if size > FEW else own.shape[::-1]
    near = []
    for (start, count), part in zip(PARTS, passed):
        low, end = max(first, start), min(first + size, start + count)
        if low < end:
            near.append((part, low - start, low - first, end - low))

    def kernel(*refs):
        near_refs, (far_ref, own_ref, _, out_ref, sem, load_sem, held, buf) = refs[:len(near)], refs[len(near):]
        p = lax.axis_index("row")

        def place(start, wide):
            return out_ref.at[0, 2, pl.ds(first, size), pl.ds(start, wide)]

        @pl.when(p == 0)
        def _():
            for ref, (_, src, dst, count) in zip(near_refs, near):
                load(ref.at[pl.ds(src, count), :], held.at[pl.ds(dst, count), :], load_sem)

        @pl.when(p == 1)
        def _():
            load(far_ref, held, load_sem)

        if size > FEW:

            @pl.when(p < 2)
            def _():
                stream(
                    rows // WIDE, buf, sem,
                    lambda s: dot_t(held[...], tiles(own_ref, s, WIDE)),
                    lambda s: place(s * WIDE, WIDE),
                )

        else:

            @pl.when(p < 2)
            def _():
                copies = []
                for k in range(rows // WIDE):
                    at = slice(k * WIDE, (k + 1) * WIDE)
                    buf[k] = jnp.dot(held[...], own_ref[:, at], preferred_element_type=jnp.float32)
                    copies.append(pltpu.make_async_copy(buf.at[k], place(k * WIDE, WIDE), sem.at[k]))
                    copies[-1].start()
                for copy in copies:
                    copy.wait()

        @pl.when(p >= 2)
        def _():
            stream(
                rows // WIDE, buf, sem,
                lambda s: jnp.zeros((size, WIDE), jnp.float32),
                lambda s: place(s * WIDE, WIDE),
            )

    bufs = DEPTH if size > FEW else rows // WIDE
    scratch = [pltpu.VMEM((size, depth), jnp.bfloat16), pltpu.VMEM((bufs, size, WIDE), jnp.float32)]
    refs = [(part, pl.ANY) for part, *_ in near] + [(far, pl.ANY), (own, pltpu.VMEM)]
    return call(kernel, size, rows, depth, out, refs, scratch)


def solution(mesh):
    assert mesh.shape["row"] == 4

    def send(a, pairs):
        return lax.ppermute(a, "row", pairs)

    def rows_of(a, chunk):
        return a[chunk[0]:chunk[0] + chunk[1]]

    def local(a):
        head = bring(a, *PARTS[0], 58 << 20)
        parts = [send(head, NEXT)]
        own = bring(a, 0, a.shape[0], 51 << 20)
        parts += [send(rows_of(own, PARTS[k]), NEXT) for k in range(1, len(PARTS))]
        out = diag(own)
        passed = [send(part, PASS) for part in parts]
        pieces = cut(own)
        far = [send(piece, FAR) for piece in pieces]
        for k, chunk in enumerate(PARTS):
            out = slot1(*chunk, parts[k], own, out)
        for j, chunk in enumerate(FARS):
            out = slot2(*chunk, passed, far[j], own if chunk[1] > FEW else turned, out)
            if j == TURN_AFTER:
                turned, out = turn(own, out)
        return out

    return jax.shard_map(
        local, mesh=mesh, in_specs=(P(("mat", "row"), None),), out_specs=P(("mat", "row"), None, None, None), check_vma=False
    )
```

```python
import jax
import jax.numpy as jnp
from jax import lax
from jax.experimental import pallas as pl
from jax.experimental.pallas import tpu as pltpu
from jax.sharding import PartitionSpec as P


WIDE = 512
HIGH = 1792
NEXT = [(1, 0), (2, 1), (3, 2), (0, 3)]
FAR = [(3, 1)]
PASS = [(1, 0)]
PARTS = [(0, 96), (96, 1952), (2048, 1024), (3072, 512)]
GROUPS = [[0, 1], [2], [3]]
FARS = [(0, 816), (816, 768), (1584, 768), (2352, 464), (2816, 272), (3088, 192), (3280, 160), (3440, 144)]
TURN_AFTER = 0
DEPTH = 3
FEW = 464


def dot_t(x, y):
    return lax.dot_general(x, y, (((1,), (1,)), ((), ())), preferred_element_type=jnp.float32)


def tiles(ref, index, size):
    return ref[pl.ds(pl.multiple_of(index * size, size), size), :]


def stream(steps, buf, sem, value, place):
    def copy(s):
        return pltpu.make_async_copy(buf.at[lax.rem(s, DEPTH)], place(s), sem.at[lax.rem(s, DEPTH)])

    @pl.loop(0, steps)
    def _(s):
        @pl.when(s >= DEPTH)
        def _():
            copy(s - DEPTH).wait()

        buf[lax.rem(s, DEPTH)] = value(s)
        copy(s).start()

    for s in range(max(steps - DEPTH, 0), steps):
        copy(s).wait()


def load(src, dst, sem):
    copy = pltpu.make_async_copy(src, dst, sem)
    copy.start()
    copy.wait()


def call(kernel, rows, cols, depth, out, refs, scratch):
    made = isinstance(out, jax.ShapeDtypeStruct)
    args = [a for a, _ in refs] + ([] if made else [out])
    return pl.pallas_call(
        kernel,
        in_specs=[pl.BlockSpec(memory_space=space) for _, space in refs] + ([] if made else [pl.BlockSpec(memory_space=pl.ANY)]),
        out_specs=pl.BlockSpec(memory_space=pl.ANY),
        out_shape=jax.ShapeDtypeStruct(out.shape, out.dtype),
        input_output_aliases={} if made else {len(args) - 1: 0},
        scratch_shapes=[pltpu.SemaphoreType.DMA((8,)), pltpu.SemaphoreType.DMA, *scratch],
        cost_estimate=pl.CostEstimate(
            flops=2 * rows * cols * depth, bytes_accessed=4 * rows * cols + 2 * rows * depth, transcendentals=0
        ),
        compiler_params=pltpu.CompilerParams(vmem_limit_bytes=32 << 20),
    )(*args)


def bring(a, first, size, grant):
    def kernel(a_ref, rows_ref, sem):
        load(a_ref.at[pl.ds(first, size), :], rows_ref, sem)

    return pl.pallas_call(
        kernel,
        in_specs=[pl.BlockSpec(memory_space=pl.ANY)],
        out_specs=pl.BlockSpec(memory_space=pltpu.VMEM),
        out_shape=pltpu.VMEM((size, a.shape[1]), a.dtype),
        scratch_shapes=[pltpu.SemaphoreType.DMA],
        cost_estimate=pl.CostEstimate(flops=0, bytes_accessed=4 * size * a.shape[1], transcendentals=0),
        compiler_params=pltpu.CompilerParams(vmem_limit_bytes=grant),
        name="bring",
    )(a)


def cut(own):
    depth = own.shape[1]

    def kernel(own_ref, *refs):
        piece_refs, sem = refs[:-1], refs[-1]

        @pl.when(lax.axis_index("row") == FAR[0][0])
        def _():
            copies = [
                pltpu.make_async_copy(own_ref.at[pl.ds(first, size), :], piece_ref, sem.at[k])
                for k, ((first, size), piece_ref) in enumerate(zip(FARS, piece_refs))
            ]
            for copy in copies:
                copy.start()
            for copy in copies:
                copy.wait()

    return pl.pallas_call(
        kernel,
        in_specs=[pl.BlockSpec(memory_space=pltpu.VMEM)],
        out_specs=[pl.BlockSpec(memory_space=pl.ANY)] * len(FARS),
        out_shape=[jax.ShapeDtypeStruct((size, depth), own.dtype) for _, size in FARS],
        scratch_shapes=[pltpu.SemaphoreType.DMA((len(FARS),))],
        cost_estimate=pl.CostEstimate(flops=0, bytes_accessed=4 * own.size, transcendentals=0),
        compiler_params=pltpu.CompilerParams(vmem_limit_bytes=32 << 20),
        name="cut",
    )(own)


def turn(own, out):
    rows, depth = own.shape

    def kernel(own_ref, _, turned_ref, out_ref):
        @pl.when(lax.axis_index("row") < 2)
        def _():
            @pl.loop(0, rows // WIDE)
            def _(s):
                turned_ref[:, pl.ds(pl.multiple_of(s * WIDE, WIDE), WIDE)] = tiles(own_ref, s, WIDE).T

    return pl.pallas_call(
        kernel,
        in_specs=[pl.BlockSpec(memory_space=pltpu.VMEM), pl.BlockSpec(memory_space=pl.ANY)],
        out_specs=[pl.BlockSpec(memory_space=pltpu.VMEM), pl.BlockSpec(memory_space=pl.ANY)],
        out_shape=[pltpu.VMEM((depth, rows), own.dtype), jax.ShapeDtypeStruct(out.shape, out.dtype)],
        input_output_aliases={1: 1},
        cost_estimate=pl.CostEstimate(flops=0, bytes_accessed=4 * own.size, transcendentals=0),
        compiler_params=pltpu.CompilerParams(vmem_limit_bytes=32 << 20),
        name="turn",
    )(own, out)


def diag(own):
    rows, depth = own.shape
    wide = rows // WIDE

    def kernel(own_ref, out_ref, sem, _, buf):
        stream(
            rows // HIGH * wide, buf, sem,
            lambda s: dot_t(tiles(own_ref, s // wide, HIGH), tiles(own_ref, lax.rem(s, wide), WIDE)),
            lambda s: out_ref.at[0, 0, pl.ds(s // wide * HIGH, HIGH), pl.ds(lax.rem(s, wide) * WIDE, WIDE)],
        )

    out = jax.ShapeDtypeStruct((1, 3, rows, rows), jnp.float32)
    return call(kernel, rows, rows, depth, out, [(own, pltpu.VMEM)], [pltpu.VMEM((DEPTH, HIGH, WIDE), jnp.float32)])


def slot1(group, parts, own, out):
    rows, depth = own.shape
    first = PARTS[group[0]][0]
    size = sum(PARTS[k][1] for k in group)
    tall = size // WIDE

    def kernel(*refs):
        part_refs, (own_ref, _, out_ref, sem, load_sem, held, buf) = refs[:len(group)], refs[len(group):]
        p = lax.axis_index("row")
        for k, part_ref in zip(group, part_refs):
            load(part_ref, held.at[pl.ds(PARTS[k][0] - first, PARTS[k][1]), :], load_sem)

        @pl.when(p < 3)
        def _():
            stream(
                rows // WIDE, buf.at[:, :size], sem,
                lambda s: dot_t(held[...], tiles(own_ref, s, WIDE)),
                lambda s: out_ref.at[0, 1, pl.ds(first, size), pl.ds(s * WIDE, WIDE)],
            )

        @pl.when(p == 3)
        def _():
            stream(
                rows // HIGH * tall, buf.at[:, :HIGH], sem,
                lambda s: dot_t(tiles(own_ref, s // tall, HIGH), tiles(held, lax.rem(s, tall), WIDE)),
                lambda s: out_ref.at[0, 1, pl.ds(s // tall * HIGH, HIGH), pl.ds(first + lax.rem(s, tall) * WIDE, WIDE)],
            )

    scratch = [pltpu.VMEM((size, depth), jnp.bfloat16), pltpu.VMEM((DEPTH, max(size, HIGH), WIDE), jnp.float32)]
    refs = [(part, pl.ANY) for part in parts] + [(own, pltpu.VMEM)]
    return call(kernel, size, rows, depth, out, refs, scratch)


def slot2(first, size, passed, far, own, out):
    rows, depth = own.shape if size > FEW else own.shape[::-1]
    near = []
    for (start, count), part in zip(PARTS, passed):
        low, end = max(first, start), min(first + size, start + count)
        if low < end:
            near.append((part, low - start, low - first, end - low))

    def kernel(*refs):
        near_refs, (far_ref, own_ref, _, out_ref, sem, load_sem, held, buf) = refs[:len(near)], refs[len(near):]
        p = lax.axis_index("row")

        def place(start, wide):
            return out_ref.at[0, 2, pl.ds(first, size), pl.ds(start, wide)]

        @pl.when(p == 0)
        def _():
            for ref, (_, src, dst, count) in zip(near_refs, near):
                load(ref.at[pl.ds(src, count), :], held.at[pl.ds(dst, count), :], load_sem)

        @pl.when(p == 1)
        def _():
            half = size // 32 * 16
            copies = [
                pltpu.make_async_copy(far_ref.at[at, :], held.at[at, :], load_sem)
                for at in (pl.ds(0, half), pl.ds(half, size - half))
            ]
            for copy in copies:
                copy.start()
            for copy in copies:
                copy.wait()

        if size > FEW:

            @pl.when(p < 2)
            def _():
                stream(
                    rows // WIDE, buf, sem,
                    lambda s: dot_t(held[...], tiles(own_ref, s, WIDE)),
                    lambda s: place(s * WIDE, WIDE),
                )

        else:

            @pl.when(p < 2)
            def _():
                copies = []
                for k in range(rows // WIDE):
                    at = slice(k * WIDE, (k + 1) * WIDE)
                    buf[k] = jnp.dot(held[...], own_ref[:, at], preferred_element_type=jnp.float32)
                    copies.append(pltpu.make_async_copy(buf.at[k], place(k * WIDE, WIDE), sem.at[k]))
                    copies[-1].start()
                for copy in copies:
                    copy.wait()

        @pl.when(p >= 2)
        def _():
            stream(
                rows // WIDE, buf, sem,
                lambda s: jnp.zeros((size, WIDE), jnp.float32),
                lambda s: place(s * WIDE, WIDE),
            )

    bufs = DEPTH if size > FEW else rows // WIDE
    scratch = [pltpu.VMEM((size, depth), jnp.bfloat16), pltpu.VMEM((bufs, size, WIDE), jnp.float32)]
    refs = [(part, pl.ANY) for part, *_ in near] + [(far, pl.ANY), (own, pltpu.VMEM)]
    return call(kernel, size, rows, depth, out, refs, scratch)


def solution(mesh):
    assert mesh.shape["row"] == 4

    def send(a, pairs):
        return lax.ppermute(a, "row", pairs)

    def rows_of(a, chunk):
        return a[chunk[0]:chunk[0] + chunk[1]]

    def local(a):
        head = bring(a, *PARTS[0], 58 << 20)
        parts = [send(head, NEXT)]
        second = bring(a, *PARTS[1], 55 << 20)
        parts += [send(second, NEXT)]
        own = bring(a, 0, a.shape[0], 51 << 20)
        parts += [send(rows_of(own, PARTS[k]), NEXT) for k in range(2, len(PARTS))]
        out = diag(own)
        passed = [send(part, PASS) for part in parts]
        pieces = cut(own)
        far = [send(piece, FAR) for piece in pieces]
        for group in GROUPS:
            out = slot1(group, [parts[k] for k in group], own, out)
        for j, chunk in enumerate(FARS):
            out = slot2(*chunk, passed, far[j], own if chunk[1] > FEW else turned, out)
            if j == TURN_AFTER:
                turned, out = turn(own, out)
        return out

    return jax.shard_map(
        local, mesh=mesh, in_specs=(P(("mat", "row"), None),), out_specs=P(("mat", "row"), None, None, None), check_vma=False
    )
```

```python
import jax
import jax.numpy as jnp
from jax import lax
from jax.experimental import pallas as pl
from jax.experimental.pallas import tpu as pltpu
from jax.sharding import PartitionSpec as P


WIDE = 512
HIGH = 1792
NEXT = [(1, 0), (2, 1), (3, 2), (0, 3)]
FAR = [(3, 1), (1, 0), (0, 2), (2, 3)]
PASS = [(1, 0)]
PARTS = [(0, 192), (192, 1856), (2048, 1024), (3072, 512)]
GROUPS = [[0, 1], [2], [3]]
FARS = [(0, 816), (816, 768), (1584, 768), (2352, 464), (2816, 272), (3088, 192), (3280, 160), (3440, 144)]
HEAD = PARTS[0][1]
SENDS = [(HEAD, FARS[0][1] - HEAD)] + FARS[1:]
DEPTH = 3
FEW = 464


def dot_t(x, y):
    return lax.dot_general(x, y, (((1,), (1,)), ((), ())), preferred_element_type=jnp.float32)


def tiles(ref, index, size):
    return ref[pl.ds(pl.multiple_of(index * size, size), size), :]


def stream(steps, buf, sem, value, place):
    def copy(s):
        return pltpu.make_async_copy(buf.at[lax.rem(s, DEPTH)], place(s), sem.at[lax.rem(s, DEPTH)])

    @pl.loop(0, steps)
    def _(s):
        @pl.when(s >= DEPTH)
        def _():
            copy(s - DEPTH).wait()

        buf[lax.rem(s, DEPTH)] = value(s)
        copy(s).start()

    for s in range(max(steps - DEPTH, 0), steps):
        copy(s).wait()


def load(src, dst, sem):
    copy = pltpu.make_async_copy(src, dst, sem)
    copy.start()
    copy.wait()


def fill(held, refs, starts, counts, sem):
    copies, at = [], 0
    for ref, start, count in zip(refs, starts, counts):
        copies.append(pltpu.make_async_copy(ref.at[pl.ds(start, count), :], held.at[pl.ds(at, count), :], sem))
        at += count
    for copy in copies:
        copy.start()
    for copy in copies:
        copy.wait()


def call(kernel, rows, cols, depth, out, refs, scratch):
    made = isinstance(out, jax.ShapeDtypeStruct)
    args = [a for a, _ in refs] + ([] if made else [out])
    return pl.pallas_call(
        kernel,
        in_specs=[pl.BlockSpec(memory_space=space) for _, space in refs] + ([] if made else [pl.BlockSpec(memory_space=pl.ANY)]),
        out_specs=pl.BlockSpec(memory_space=pl.ANY),
        out_shape=jax.ShapeDtypeStruct(out.shape, out.dtype),
        input_output_aliases={} if made else {len(args) - 1: 0},
        scratch_shapes=[pltpu.SemaphoreType.DMA((8,)), pltpu.SemaphoreType.DMA, *scratch],
        cost_estimate=pl.CostEstimate(
            flops=2 * rows * cols * depth, bytes_accessed=4 * rows * cols + 2 * rows * depth, transcendentals=0
        ),
        compiler_params=pltpu.CompilerParams(vmem_limit_bytes=32 << 20),
    )(*args)


def bring(a, first, size, grant):
    def kernel(a_ref, rows_ref, sem):
        load(a_ref.at[pl.ds(first, size), :], rows_ref, sem)

    return pl.pallas_call(
        kernel,
        in_specs=[pl.BlockSpec(memory_space=pl.ANY)],
        out_specs=pl.BlockSpec(memory_space=pltpu.VMEM),
        out_shape=pltpu.VMEM((size, a.shape[1]), a.dtype),
        scratch_shapes=[pltpu.SemaphoreType.DMA],
        cost_estimate=pl.CostEstimate(flops=0, bytes_accessed=4 * size * a.shape[1], transcendentals=0),
        compiler_params=pltpu.CompilerParams(vmem_limit_bytes=grant),
        name="bring",
    )(a)


def cut(own):
    depth = own.shape[1]

    def kernel(own_ref, *refs):
        piece_refs, sem = refs[:-1], refs[-1]

        @pl.when(lax.axis_index("row") == FAR[0][0])
        def _():
            copies = [
                pltpu.make_async_copy(own_ref.at[pl.ds(first, size), :], piece_ref, sem.at[k])
                for k, ((first, size), piece_ref) in enumerate(zip(SENDS, piece_refs))
            ]
            for copy in copies:
                copy.start()
            for copy in copies:
                copy.wait()

    return pl.pallas_call(
        kernel,
        in_specs=[pl.BlockSpec(memory_space=pltpu.VMEM)],
        out_specs=[pl.BlockSpec(memory_space=pl.ANY)] * len(SENDS),
        out_shape=[jax.ShapeDtypeStruct((size, depth), own.dtype) for _, size in SENDS],
        scratch_shapes=[pltpu.SemaphoreType.DMA((len(SENDS),))],
        cost_estimate=pl.CostEstimate(flops=0, bytes_accessed=4 * own.size, transcendentals=0),
        compiler_params=pltpu.CompilerParams(vmem_limit_bytes=32 << 20),
        name="cut",
    )(own)


def turn(own, out):
    rows, depth = own.shape

    def kernel(own_ref, _, turned_ref, out_ref):
        @pl.when(lax.axis_index("row") < 2)
        def _():
            @pl.loop(0, rows // WIDE)
            def _(s):
                turned_ref[:, pl.ds(pl.multiple_of(s * WIDE, WIDE), WIDE)] = tiles(own_ref, s, WIDE).T

    return pl.pallas_call(
        kernel,
        in_specs=[pl.BlockSpec(memory_space=pltpu.VMEM), pl.BlockSpec(memory_space=pl.ANY)],
        out_specs=[pl.BlockSpec(memory_space=pltpu.VMEM), pl.BlockSpec(memory_space=pl.ANY)],
        out_shape=[pltpu.VMEM((depth, rows), own.dtype), jax.ShapeDtypeStruct(out.shape, out.dtype)],
        input_output_aliases={1: 1},
        cost_estimate=pl.CostEstimate(flops=0, bytes_accessed=4 * own.size, transcendentals=0),
        compiler_params=pltpu.CompilerParams(vmem_limit_bytes=32 << 20),
        name="turn",
    )(own, out)


def diag(own):
    rows, depth = own.shape
    wide = rows // WIDE

    def kernel(own_ref, out_ref, sem, _, buf):
        stream(
            rows // HIGH * wide, buf, sem,
            lambda s: dot_t(tiles(own_ref, s // wide, HIGH), tiles(own_ref, lax.rem(s, wide), WIDE)),
            lambda s: out_ref.at[0, 0, pl.ds(s // wide * HIGH, HIGH), pl.ds(lax.rem(s, wide) * WIDE, WIDE)],
        )

    out = jax.ShapeDtypeStruct((1, 3, rows, rows), jnp.float32)
    return call(kernel, rows, rows, depth, out, [(own, pltpu.VMEM)], [pltpu.VMEM((DEPTH, HIGH, WIDE), jnp.float32)])


def slot1(group, parts, own, out):
    rows, depth = own.shape
    first = PARTS[group[0]][0]
    size = sum(PARTS[k][1] for k in group)
    tall = size // WIDE

    def kernel(*refs):
        part_refs, (own_ref, _, out_ref, sem, load_sem, held, buf) = refs[:len(group)], refs[len(group):]
        p = lax.axis_index("row")
        fill(held, part_refs, [0] * len(group), [PARTS[k][1] for k in group], load_sem)

        @pl.when(p < 3)
        def _():
            stream(
                rows // WIDE, buf.at[:, :size], sem,
                lambda s: dot_t(held[...], tiles(own_ref, s, WIDE)),
                lambda s: out_ref.at[0, 1, pl.ds(first, size), pl.ds(s * WIDE, WIDE)],
            )

        @pl.when(p == 3)
        def _():
            stream(
                rows // HIGH * tall, buf.at[:, :HIGH], sem,
                lambda s: dot_t(tiles(own_ref, s // tall, HIGH), tiles(held, lax.rem(s, tall), WIDE)),
                lambda s: out_ref.at[0, 1, pl.ds(s // tall * HIGH, HIGH), pl.ds(first + lax.rem(s, tall) * WIDE, WIDE)],
            )

    scratch = [pltpu.VMEM((size, depth), jnp.bfloat16), pltpu.VMEM((DEPTH, max(size, HIGH), WIDE), jnp.float32)]
    refs = [(part, pl.ANY) for part in parts] + [(own, pltpu.VMEM)]
    return call(kernel, size, rows, depth, out, refs, scratch)


def slot2(first, size, passed, far, own, out):
    rows, depth = own.shape if size > FEW else own.shape[::-1]
    near = []
    for (start, count), part in zip(PARTS, passed):
        low, end = max(first, start), min(first + size, start + count)
        if low < end:
            near.append((part, low - start, end - low))

    def kernel(*refs):
        near_refs, far_refs = refs[:len(near)], refs[len(near):len(near) + len(far)]
        own_ref, _, out_ref, sem, load_sem, held, buf = refs[len(near) + len(far):]
        p = lax.axis_index("row")

        def place(start, wide):
            return out_ref.at[0, 2, pl.ds(first, size), pl.ds(start, wide)]

        @pl.when(p == 0)
        def _():
            fill(held, near_refs, [src for _, src, _ in near], [count for _, _, count in near], load_sem)

        @pl.when(p == 1)
        def _():
            if len(far) > 1:
                held[:HEAD, :] = far_refs[0][...]
            load(far_refs[-1], held.at[pl.ds(size - far[-1].shape[0], far[-1].shape[0]), :], load_sem)

        if size > FEW:

            @pl.when(p < 2)
            def _():
                stream(
                    rows // WIDE, buf, sem,
                    lambda s: dot_t(held[...], tiles(own_ref, s, WIDE)),
                    lambda s: place(s * WIDE, WIDE),
                )

        else:

            @pl.when(p < 2)
            def _():
                copies = []
                for k in range(rows // WIDE):
                    at = slice(k * WIDE, (k + 1) * WIDE)
                    buf[k] = jnp.dot(held[...], own_ref[:, at], preferred_element_type=jnp.float32)
                    copies.append(pltpu.make_async_copy(buf.at[k], place(k * WIDE, WIDE), sem.at[k]))
                    copies[-1].start()
                for copy in copies:
                    copy.wait()

        @pl.when(p >= 2)
        def _():
            stream(
                rows // WIDE, buf, sem,
                lambda s: jnp.zeros((size, WIDE), jnp.float32),
                lambda s: place(s * WIDE, WIDE),
            )

    bufs = DEPTH if size > FEW else rows // WIDE
    scratch = [pltpu.VMEM((size, depth), jnp.bfloat16), pltpu.VMEM((bufs, size, WIDE), jnp.float32)]
    refs = [(part, pl.ANY) for part, *_ in near] + [(part, pltpu.VMEM) for part in far[:-1]] + [(far[-1], pl.ANY), (own, pltpu.VMEM)]
    return call(kernel, size, rows, depth, out, refs, scratch)


def solution(mesh):
    assert mesh.shape["row"] == 4

    def send(a, pairs):
        return lax.ppermute(a, "row", pairs)

    def rows_of(a, chunk):
        return a[chunk[0]:chunk[0] + chunk[1]]

    def local(a):
        head = bring(a, *PARTS[0], 58 << 20)
        far_head = send(head, FAR)
        parts = [send(head, NEXT)]
        own = bring(a, 0, a.shape[0], 51 << 20)
        parts += [send(rows_of(own, PARTS[k]), NEXT) for k in range(1, len(PARTS))]
        out = diag(own)
        passed = [send(part, PASS) for part in parts]
        pieces = cut(own)
        far = [[send(piece, FAR)] for piece in pieces]
        far[0].insert(0, far_head)
        turned, out = turn(own, out)
        for group in GROUPS:
            out = slot1(group, [parts[k] for k in group], own, out)
        for j, chunk in enumerate(FARS):
            out = slot2(*chunk, passed, far[j], own if chunk[1] > FEW else turned, out)
        return out

    return jax.shard_map(
        local, mesh=mesh, in_specs=(P(("mat", "row"), None),), out_specs=P(("mat", "row"), None, None, None), check_vma=False
    )
```

```python
import jax
import jax.numpy as jnp
from jax import lax
from jax.experimental import pallas as pl
from jax.experimental.pallas import tpu as pltpu
from jax.sharding import PartitionSpec as P


WIDE = 512
HIGH = 1792
NEXT = [(1, 0), (2, 1), (3, 2), (0, 3)]
FAR = [(3, 1)]
FAR_HEAD = [(3, 1), (1, 0), (0, 2), (2, 3)]
PASS = [(1, 0)]
PARTS = [(0, 192), (192, 1856), (2048, 1024), (3072, 512)]
GROUPS = [[0, 1], [2], [3]]
FARS = [(0, 816), (816, 768), (1584, 768), (2352, 464), (2816, 272), (3088, 192), (3280, 160), (3440, 144)]
HEAD = PARTS[0][1]
SENDS = [(HEAD, FARS[0][1] - HEAD)] + FARS[1:]
DEPTH = 3
FEW = 464


def dot_t(x, y):
    return lax.dot_general(x, y, (((1,), (1,)), ((), ())), preferred_element_type=jnp.float32)


def tiles(ref, index, size):
    return ref[pl.ds(pl.multiple_of(index * size, size), size), :]


def stream(steps, buf, sem, value, place):
    def copy(s):
        return pltpu.make_async_copy(buf.at[lax.rem(s, DEPTH)], place(s), sem.at[lax.rem(s, DEPTH)])

    @pl.loop(0, steps)
    def _(s):
        @pl.when(s >= DEPTH)
        def _():
            copy(s - DEPTH).wait()

        buf[lax.rem(s, DEPTH)] = value(s)
        copy(s).start()

    for s in range(max(steps - DEPTH, 0), steps):
        copy(s).wait()


def load(src, dst, sem):
    copy = pltpu.make_async_copy(src, dst, sem)
    copy.start()
    copy.wait()


def fill(held, refs, starts, counts, sem):
    copies, at = [], 0
    for ref, start, count in zip(refs, starts, counts):
        copies.append(pltpu.make_async_copy(ref.at[pl.ds(start, count), :], held.at[pl.ds(at, count), :], sem))
        at += count
    for copy in copies:
        copy.start()
    for copy in copies:
        copy.wait()


def call(kernel, rows, cols, depth, out, refs, scratch):
    made = isinstance(out, jax.ShapeDtypeStruct)
    args = [a for a, _ in refs] + ([] if made else [out])
    return pl.pallas_call(
        kernel,
        in_specs=[pl.BlockSpec(memory_space=space) for _, space in refs] + ([] if made else [pl.BlockSpec(memory_space=pl.ANY)]),
        out_specs=pl.BlockSpec(memory_space=pl.ANY),
        out_shape=jax.ShapeDtypeStruct(out.shape, out.dtype),
        input_output_aliases={} if made else {len(args) - 1: 0},
        scratch_shapes=[pltpu.SemaphoreType.DMA((8,)), pltpu.SemaphoreType.DMA, *scratch],
        cost_estimate=pl.CostEstimate(
            flops=2 * rows * cols * depth, bytes_accessed=4 * rows * cols + 2 * rows * depth, transcendentals=0
        ),
        compiler_params=pltpu.CompilerParams(vmem_limit_bytes=32 << 20),
    )(*args)


def bring(a, first, size, grant):
    def kernel(a_ref, rows_ref, sem):
        load(a_ref.at[pl.ds(first, size), :], rows_ref, sem)

    return pl.pallas_call(
        kernel,
        in_specs=[pl.BlockSpec(memory_space=pl.ANY)],
        out_specs=pl.BlockSpec(memory_space=pltpu.VMEM),
        out_shape=pltpu.VMEM((size, a.shape[1]), a.dtype),
        scratch_shapes=[pltpu.SemaphoreType.DMA],
        cost_estimate=pl.CostEstimate(flops=0, bytes_accessed=4 * size * a.shape[1], transcendentals=0),
        compiler_params=pltpu.CompilerParams(vmem_limit_bytes=grant),
        name="bring",
    )(a)


def cut(own):
    depth = own.shape[1]

    def kernel(own_ref, *refs):
        piece_refs, sem = refs[:-1], refs[-1]

        @pl.when(lax.axis_index("row") == FAR[0][0])
        def _():
            copies = [
                pltpu.make_async_copy(own_ref.at[pl.ds(first, size), :], piece_ref, sem.at[k])
                for k, ((first, size), piece_ref) in enumerate(zip(SENDS, piece_refs))
            ]
            for copy in copies:
                copy.start()
            for copy in copies:
                copy.wait()

    return pl.pallas_call(
        kernel,
        in_specs=[pl.BlockSpec(memory_space=pltpu.VMEM)],
        out_specs=[pl.BlockSpec(memory_space=pl.ANY)] * len(SENDS),
        out_shape=[jax.ShapeDtypeStruct((size, depth), own.dtype) for _, size in SENDS],
        scratch_shapes=[pltpu.SemaphoreType.DMA((len(SENDS),))],
        cost_estimate=pl.CostEstimate(flops=0, bytes_accessed=4 * own.size, transcendentals=0),
        compiler_params=pltpu.CompilerParams(vmem_limit_bytes=32 << 20),
        name="cut",
    )(own)


def turn(own, out):
    rows, depth = own.shape

    def kernel(own_ref, _, turned_ref, out_ref):
        @pl.when(lax.axis_index("row") < 2)
        def _():
            @pl.loop(0, rows // WIDE)
            def _(s):
                turned_ref[:, pl.ds(pl.multiple_of(s * WIDE, WIDE), WIDE)] = tiles(own_ref, s, WIDE).T

    return pl.pallas_call(
        kernel,
        in_specs=[pl.BlockSpec(memory_space=pltpu.VMEM), pl.BlockSpec(memory_space=pl.ANY)],
        out_specs=[pl.BlockSpec(memory_space=pltpu.VMEM), pl.BlockSpec(memory_space=pl.ANY)],
        out_shape=[pltpu.VMEM((depth, rows), own.dtype), jax.ShapeDtypeStruct(out.shape, out.dtype)],
        input_output_aliases={1: 1},
        cost_estimate=pl.CostEstimate(flops=0, bytes_accessed=4 * own.size, transcendentals=0),
        compiler_params=pltpu.CompilerParams(vmem_limit_bytes=32 << 20),
        name="turn",
    )(own, out)


def diag(own):
    rows, depth = own.shape
    wide = rows // WIDE

    def kernel(own_ref, out_ref, sem, _, buf):
        stream(
            rows // HIGH * wide, buf, sem,
            lambda s: dot_t(tiles(own_ref, s // wide, HIGH), tiles(own_ref, lax.rem(s, wide), WIDE)),
            lambda s: out_ref.at[0, 0, pl.ds(s // wide * HIGH, HIGH), pl.ds(lax.rem(s, wide) * WIDE, WIDE)],
        )

    out = jax.ShapeDtypeStruct((1, 3, rows, rows), jnp.float32)
    return call(kernel, rows, rows, depth, out, [(own, pltpu.VMEM)], [pltpu.VMEM((DEPTH, HIGH, WIDE), jnp.float32)])


def slot1(group, parts, own, out):
    rows, depth = own.shape
    first = PARTS[group[0]][0]
    size = sum(PARTS[k][1] for k in group)
    tall = size // WIDE

    def kernel(*refs):
        part_refs, (own_ref, _, out_ref, sem, load_sem, held, buf) = refs[:len(group)], refs[len(group):]
        p = lax.axis_index("row")
        fill(held, part_refs, [0] * len(group), [PARTS[k][1] for k in group], load_sem)

        @pl.when(p < 3)
        def _():
            stream(
                rows // WIDE, buf.at[:, :size], sem,
                lambda s: dot_t(held[...], tiles(own_ref, s, WIDE)),
                lambda s: out_ref.at[0, 1, pl.ds(first, size), pl.ds(s * WIDE, WIDE)],
            )

        @pl.when(p == 3)
        def _():
            stream(
                rows // HIGH * tall, buf.at[:, :HIGH], sem,
                lambda s: dot_t(tiles(own_ref, s // tall, HIGH), tiles(held, lax.rem(s, tall), WIDE)),
                lambda s: out_ref.at[0, 1, pl.ds(s // tall * HIGH, HIGH), pl.ds(first + lax.rem(s, tall) * WIDE, WIDE)],
            )

    scratch = [pltpu.VMEM((size, depth), jnp.bfloat16), pltpu.VMEM((DEPTH, max(size, HIGH), WIDE), jnp.float32)]
    refs = [(part, pl.ANY) for part in parts] + [(own, pltpu.VMEM)]
    return call(kernel, size, rows, depth, out, refs, scratch)


def slot2(first, size, passed, far, own, out):
    rows, depth = own.shape if size > FEW else own.shape[::-1]
    near = []
    for (start, count), part in zip(PARTS, passed):
        low, end = max(first, start), min(first + size, start + count)
        if low < end:
            near.append((part, low - start, end - low))

    def kernel(*refs):
        near_refs, far_refs = refs[:len(near)], refs[len(near):len(near) + len(far)]
        own_ref, _, out_ref, sem, load_sem, held, buf = refs[len(near) + len(far):]
        p = lax.axis_index("row")

        def place(start, wide):
            return out_ref.at[0, 2, pl.ds(first, size), pl.ds(start, wide)]

        @pl.when(p == 0)
        def _():
            fill(held, near_refs, [src for _, src, _ in near], [count for _, _, count in near], load_sem)

        @pl.when(p == 1)
        def _():
            if len(far) > 1:
                held[:HEAD, :] = far_refs[0][...]
            load(far_refs[-1], held.at[pl.ds(size - far[-1].shape[0], far[-1].shape[0]), :], load_sem)

        if size > FEW:

            @pl.when(p < 2)
            def _():
                stream(
                    rows // WIDE, buf, sem,
                    lambda s: dot_t(held[...], tiles(own_ref, s, WIDE)),
                    lambda s: place(s * WIDE, WIDE),
                )

        else:

            @pl.when(p < 2)
            def _():
                copies = []
                for k in range(rows // WIDE):
                    at = slice(k * WIDE, (k + 1) * WIDE)
                    buf[k] = jnp.dot(held[...], own_ref[:, at], preferred_element_type=jnp.float32)
                    copies.append(pltpu.make_async_copy(buf.at[k], place(k * WIDE, WIDE), sem.at[k]))
                    copies[-1].start()
                for copy in copies:
                    copy.wait()

        @pl.when(p >= 2)
        def _():
            stream(
                rows // WIDE, buf, sem,
                lambda s: jnp.zeros((size, WIDE), jnp.float32),
                lambda s: place(s * WIDE, WIDE),
            )

    bufs = DEPTH if size > FEW else rows // WIDE
    scratch = [pltpu.VMEM((size, depth), jnp.bfloat16), pltpu.VMEM((bufs, size, WIDE), jnp.float32)]
    refs = [(part, pl.ANY) for part, *_ in near] + [(part, pltpu.VMEM) for part in far[:-1]] + [(far[-1], pl.ANY), (own, pltpu.VMEM)]
    return call(kernel, size, rows, depth, out, refs, scratch)


def solution(mesh):
    assert mesh.shape["row"] == 4

    def send(a, pairs):
        return lax.ppermute(a, "row", pairs)

    def rows_of(a, chunk):
        return a[chunk[0]:chunk[0] + chunk[1]]

    def local(a):
        head = bring(a, *PARTS[0], 58 << 20)
        far_head = send(head, FAR_HEAD)
        parts = [send(head, NEXT)]
        own = bring(a, 0, a.shape[0], 51 << 20)
        parts += [send(rows_of(own, PARTS[k]), NEXT) for k in range(1, len(PARTS))]
        out = diag(own)
        passed = [send(part, PASS) for part in parts]
        pieces = cut(own)
        far = [[send(piece, FAR)] for piece in pieces]
        far[0].insert(0, far_head)
        turned, out = turn(own, out)
        for group in GROUPS:
            out = slot1(group, [parts[k] for k in group], own, out)
        for j, chunk in enumerate(FARS):
            out = slot2(*chunk, passed, far[j], own if chunk[1] > FEW else turned, out)
        return out

    return jax.shard_map(
        local, mesh=mesh, in_specs=(P(("mat", "row"), None),), out_specs=P(("mat", "row"), None, None, None), check_vma=False
    )
```

```python
import jax
import jax.numpy as jnp
from jax import lax
from jax.experimental import pallas as pl
from jax.experimental.pallas import tpu as pltpu
from jax.sharding import PartitionSpec as P


WIDE = 512
HIGH = 1792
NEXT = [(1, 0), (2, 1), (3, 2), (0, 3)]
FAR = [(3, 1)]
FAR_HEAD = [(3, 1), (1, 0), (0, 2), (2, 3)]
PASS = [(1, 0)]
PARTS = [(0, 144), (144, 1904), (2048, 1024), (3072, 512)]
GROUPS = [[0, 1], [2, 3]]
FARS = [(0, 816), (816, 768), (1584, 768), (2352, 464), (2816, 272), (3088, 192), (3280, 160), (3440, 144)]
HEAD = PARTS[0][1]
SENDS = [(HEAD, FARS[0][1] - HEAD)] + FARS[1:]
DEPTH = 3
FEW = 464


def dot_t(x, y):
    return lax.dot_general(x, y, (((1,), (1,)), ((), ())), preferred_element_type=jnp.float32)


def tiles(ref, index, size):
    return ref[pl.ds(pl.multiple_of(index * size, size), size), :]


def stream(steps, buf, sem, value, place):
    def copy(s):
        return pltpu.make_async_copy(buf.at[lax.rem(s, DEPTH)], place(s), sem.at[lax.rem(s, DEPTH)])

    @pl.loop(0, steps)
    def _(s):
        @pl.when(s >= DEPTH)
        def _():
            copy(s - DEPTH).wait()

        buf[lax.rem(s, DEPTH)] = value(s)
        copy(s).start()

    for s in range(max(steps - DEPTH, 0), steps):
        copy(s).wait()


def load(src, dst, sem):
    copy = pltpu.make_async_copy(src, dst, sem)
    copy.start()
    copy.wait()


def fill(held, refs, starts, counts, sem):
    copies, at = [], 0
    for ref, start, count in zip(refs, starts, counts):
        copies.append(pltpu.make_async_copy(ref.at[pl.ds(start, count), :], held.at[pl.ds(at, count), :], sem))
        at += count
    for copy in copies:
        copy.start()
    for copy in copies:
        copy.wait()


def call(kernel, rows, cols, depth, out, refs, scratch):
    made = isinstance(out, jax.ShapeDtypeStruct)
    args = [a for a, _ in refs] + ([] if made else [out])
    return pl.pallas_call(
        kernel,
        in_specs=[pl.BlockSpec(memory_space=space) for _, space in refs] + ([] if made else [pl.BlockSpec(memory_space=pl.ANY)]),
        out_specs=pl.BlockSpec(memory_space=pl.ANY),
        out_shape=jax.ShapeDtypeStruct(out.shape, out.dtype),
        input_output_aliases={} if made else {len(args) - 1: 0},
        scratch_shapes=[pltpu.SemaphoreType.DMA((8,)), pltpu.SemaphoreType.DMA, *scratch],
        cost_estimate=pl.CostEstimate(
            flops=2 * rows * cols * depth, bytes_accessed=4 * rows * cols + 2 * rows * depth, transcendentals=0
        ),
        compiler_params=pltpu.CompilerParams(vmem_limit_bytes=32 << 20),
    )(*args)


def bring(a, first, size, grant):
    def kernel(a_ref, rows_ref, sem):
        load(a_ref.at[pl.ds(first, size), :], rows_ref, sem)

    return pl.pallas_call(
        kernel,
        in_specs=[pl.BlockSpec(memory_space=pl.ANY)],
        out_specs=pl.BlockSpec(memory_space=pltpu.VMEM),
        out_shape=pltpu.VMEM((size, a.shape[1]), a.dtype),
        scratch_shapes=[pltpu.SemaphoreType.DMA],
        cost_estimate=pl.CostEstimate(flops=0, bytes_accessed=4 * size * a.shape[1], transcendentals=0),
        compiler_params=pltpu.CompilerParams(vmem_limit_bytes=grant),
        name="bring",
    )(a)


def cut(own):
    depth = own.shape[1]

    def kernel(own_ref, *refs):
        piece_refs, sem = refs[:-1], refs[-1]

        @pl.when(lax.axis_index("row") == FAR[0][0])
        def _():
            copies = [
                pltpu.make_async_copy(own_ref.at[pl.ds(first, size), :], piece_ref, sem.at[k])
                for k, ((first, size), piece_ref) in enumerate(zip(SENDS, piece_refs))
            ]
            for copy in copies:
                copy.start()
            for copy in copies:
                copy.wait()

    return pl.pallas_call(
        kernel,
        in_specs=[pl.BlockSpec(memory_space=pltpu.VMEM)],
        out_specs=[pl.BlockSpec(memory_space=pl.ANY)] * len(SENDS),
        out_shape=[jax.ShapeDtypeStruct((size, depth), own.dtype) for _, size in SENDS],
        scratch_shapes=[pltpu.SemaphoreType.DMA((len(SENDS),))],
        cost_estimate=pl.CostEstimate(flops=0, bytes_accessed=4 * own.size, transcendentals=0),
        compiler_params=pltpu.CompilerParams(vmem_limit_bytes=32 << 20),
        name="cut",
    )(own)


def turn(own, out):
    rows, depth = own.shape

    def kernel(own_ref, _, turned_ref, out_ref):
        @pl.when(lax.axis_index("row") < 2)
        def _():
            @pl.loop(0, rows // WIDE)
            def _(s):
                turned_ref[:, pl.ds(pl.multiple_of(s * WIDE, WIDE), WIDE)] = tiles(own_ref, s, WIDE).T

    return pl.pallas_call(
        kernel,
        in_specs=[pl.BlockSpec(memory_space=pltpu.VMEM), pl.BlockSpec(memory_space=pl.ANY)],
        out_specs=[pl.BlockSpec(memory_space=pltpu.VMEM), pl.BlockSpec(memory_space=pl.ANY)],
        out_shape=[pltpu.VMEM((depth, rows), own.dtype), jax.ShapeDtypeStruct(out.shape, out.dtype)],
        input_output_aliases={1: 1},
        cost_estimate=pl.CostEstimate(flops=0, bytes_accessed=4 * own.size, transcendentals=0),
        compiler_params=pltpu.CompilerParams(vmem_limit_bytes=32 << 20),
        name="turn",
    )(own, out)


def diag(own):
    rows, depth = own.shape
    wide = rows // WIDE

    def kernel(own_ref, out_ref, sem, _, buf):
        stream(
            rows // HIGH * wide, buf, sem,
            lambda s: dot_t(tiles(own_ref, s // wide, HIGH), tiles(own_ref, lax.rem(s, wide), WIDE)),
            lambda s: out_ref.at[0, 0, pl.ds(s // wide * HIGH, HIGH), pl.ds(lax.rem(s, wide) * WIDE, WIDE)],
        )

    out = jax.ShapeDtypeStruct((1, 3, rows, rows), jnp.float32)
    return call(kernel, rows, rows, depth, out, [(own, pltpu.VMEM)], [pltpu.VMEM((DEPTH, HIGH, WIDE), jnp.float32)])


def slot1(group, parts, own, out):
    rows, depth = own.shape
    first = PARTS[group[0]][0]
    size = sum(PARTS[k][1] for k in group)
    tall = size // WIDE

    def kernel(*refs):
        part_refs, (own_ref, _, out_ref, sem, load_sem, held, buf) = refs[:len(group)], refs[len(group):]
        p = lax.axis_index("row")
        fill(held, part_refs, [0] * len(group), [PARTS[k][1] for k in group], load_sem)

        @pl.when(p < 3)
        def _():
            stream(
                rows // WIDE, buf.at[:, :size], sem,
                lambda s: dot_t(held[...], tiles(own_ref, s, WIDE)),
                lambda s: out_ref.at[0, 1, pl.ds(first, size), pl.ds(s * WIDE, WIDE)],
            )

        @pl.when(p == 3)
        def _():
            stream(
                rows // HIGH * tall, buf.at[:, :HIGH], sem,
                lambda s: dot_t(tiles(own_ref, s // tall, HIGH), tiles(held, lax.rem(s, tall), WIDE)),
                lambda s: out_ref.at[0, 1, pl.ds(s // tall * HIGH, HIGH), pl.ds(first + lax.rem(s, tall) * WIDE, WIDE)],
            )

    scratch = [pltpu.VMEM((size, depth), jnp.bfloat16), pltpu.VMEM((DEPTH, max(size, HIGH), WIDE), jnp.float32)]
    refs = [(part, pl.ANY) for part in parts] + [(own, pltpu.VMEM)]
    return call(kernel, size, rows, depth, out, refs, scratch)


def slot2(first, size, passed, far, own, out):
    rows, depth = own.shape if size > FEW else own.shape[::-1]
    near = []
    for (start, count), part in zip(PARTS, passed):
        low, end = max(first, start), min(first + size, start + count)
        if low < end:
            near.append((part, low - start, end - low))

    def kernel(*refs):
        near_refs, far_refs = refs[:len(near)], refs[len(near):len(near) + len(far)]
        own_ref, _, out_ref, sem, load_sem, held, buf = refs[len(near) + len(far):]
        p = lax.axis_index("row")

        def place(start, wide):
            return out_ref.at[0, 2, pl.ds(first, size), pl.ds(start, wide)]

        @pl.when(p == 0)
        def _():
            fill(held, near_refs, [src for _, src, _ in near], [count for _, _, count in near], load_sem)

        @pl.when(p == 1)
        def _():
            if len(far) > 1:
                held[:HEAD, :] = far_refs[0][...]
                held[HEAD:, :] = far_refs[1][...]
            else:
                load(far_refs[0], held, load_sem)

        if size > FEW:

            @pl.when(p < 2)
            def _():
                stream(
                    rows // WIDE, buf, sem,
                    lambda s: dot_t(held[...], tiles(own_ref, s, WIDE)),
                    lambda s: place(s * WIDE, WIDE),
                )

        else:

            @pl.when(p < 2)
            def _():
                copies = []
                for k in range(rows // WIDE):
                    at = slice(k * WIDE, (k + 1) * WIDE)
                    buf[k] = jnp.dot(held[...], own_ref[:, at], preferred_element_type=jnp.float32)
                    copies.append(pltpu.make_async_copy(buf.at[k], place(k * WIDE, WIDE), sem.at[k]))
                    copies[-1].start()
                for copy in copies:
                    copy.wait()

        @pl.when(p >= 2)
        def _():
            stream(
                rows // WIDE, buf, sem,
                lambda s: jnp.zeros((size, WIDE), jnp.float32),
                lambda s: place(s * WIDE, WIDE),
            )

    bufs = DEPTH if size > FEW else rows // WIDE
    scratch = [pltpu.VMEM((size, depth), jnp.bfloat16), pltpu.VMEM((bufs, size, WIDE), jnp.float32)]
    refs = [(part, pl.ANY) for part, *_ in near] + [(part, pltpu.VMEM if len(far) > 1 else pl.ANY) for part in far] + [(own, pltpu.VMEM)]
    return call(kernel, size, rows, depth, out, refs, scratch)


def solution(mesh):
    assert mesh.shape["row"] == 4

    def send(a, pairs):
        return lax.ppermute(a, "row", pairs)

    def rows_of(a, chunk):
        return a[chunk[0]:chunk[0] + chunk[1]]

    def local(a):
        head = bring(a, *PARTS[0], 58 << 20)
        far_head = send(head, FAR_HEAD)
        parts = [send(head, NEXT)]
        own = bring(a, 0, a.shape[0], 51 << 20)
        parts += [send(rows_of(own, PARTS[k]), NEXT) for k in range(1, len(PARTS))]
        out = diag(own)
        passed = [send(part, PASS) for part in parts]
        pieces = cut(own)
        far = [[send(piece, FAR)] for piece in pieces]
        far[0].insert(0, far_head)
        turned, out = turn(own, out)
        for group in GROUPS:
            out = slot1(group, [parts[k] for k in group], own, out)
        for j, chunk in enumerate(FARS):
            out = slot2(*chunk, passed, far[j], own if chunk[1] > FEW else turned, out)
        return out

    return jax.shard_map(
        local, mesh=mesh, in_specs=(P(("mat", "row"), None),), out_specs=P(("mat", "row"), None, None, None), check_vma=False
    )
```
